32 devices in a mesh: data: 2 (over x), outer: 4 (over z), expert: 4 (over y, core).
Axes of the slice: x: 2, y: 2, z: 4, core: 2. Of those that a mesh axis runs over, the one named last changes fastest.
Arguments:
- x_disp: bfloat16 [32, 128, 8, 2048], P('data', ('outer', 'expert')), parts along dimension 0
- w_gate: bfloat16 [128, 2048, 768], P(('outer', 'expert'))
- w_up: bfloat16 [128, 2048, 768], P(('outer', 'expert'))
- w_down: bfloat16 [128, 768, 2048], P(('outer', 'expert'))
- slot_idx: int32 [4096, 8], P(('data', 'outer', 'expert')), parts along dimension 0
- expert_ids: int32 [4096, 8], P(('data', 'outer', 'expert')), parts along dimension 0
- gate_wts: float32 [4096, 8], P(('data', 'outer', 'expert')), parts along dimension 0
Outputs:
- output: bfloat16 [4096, 2048], P(('data', 'outer', 'expert')), parts along dimension 0
There are 2 independent parts. The reference program is written for one: setup_inputs(seed, part) draws one part's arguments, and reference() takes and returns one part's arrays. A program takes and returns all parts, laid end to end along the dimension named above; an argument that names none is the same for every part.
All inputs are finite; a program needn't handle non-finite values.
Results may differ from the reference program's by a relative error of at most 0.00824751.
Values are sent between devices in bfloat16 or wider.
A program may use at most 1 GiB of HBM per device.

```python
import jax
import jax.numpy as jnp
from jax import lax

D = 2048
FF = 768
EXPERTS = 128
TOP = 8
CAP = 8
OUTER = 4
INNER = 4
NODE_MAX = 2
TOK = 128

GROUP_DEVS = OUTER * INNER
TOKENS = GROUP_DEVS * TOK
BLOCK_EXPERTS = EXPERTS // OUTER
BONUS = 2 ** 20


def draw_routing(key):
    key_hot, key_block, key_noise, key_bias = jax.random.split(key, 4)
    hot_expert = jax.random.randint(key_hot, (), 0, EXPERTS)
    forced = (jnp.arange(TOKENS) % TOK < CAP)[:, None]
    blocks = jnp.arange(OUTER)
    block_score = jax.random.randint(key_block, (TOKENS, OUTER), 0, 1024) * OUTER + blocks
    block_score = block_score + jnp.where(forced & (blocks == hot_expert // BLOCK_EXPERTS), BONUS, 0)
    best_blocks = jnp.argsort(-block_score, axis=1)[:, :NODE_MAX]
    chosen = jnp.any(best_blocks[:, :, None] == blocks[None, None, :], axis=1)
    experts = jnp.arange(EXPERTS)
    expert_bias = jax.random.randint(key_bias, (EXPERTS,), 0, 1024)
    rand_noise = jax.random.randint(key_noise, (TOKENS, EXPERTS), 0, 1024)
    expert_score = ((rand_noise + expert_bias) * EXPERTS + experts).reshape(TOKENS, OUTER, BLOCK_EXPERTS)
    block_best = expert_score == jnp.max(expert_score, axis=2, keepdims=True)
    expert_score = jnp.where(chosen[:, :, None], expert_score + jnp.where(block_best, BONUS, 0), -1)
    expert_score = expert_score.reshape(TOKENS, EXPERTS) + jnp.where(forced & (experts == hot_expert), 2 * BONUS, 0)
    expert_ids = jnp.sort(jnp.argsort(-expert_score, axis=1)[:, :TOP], axis=1)
    source = jnp.arange(TOKENS) // TOK
    group_id = (source[:, None] * EXPERTS + expert_ids).reshape(-1)
    sort_order = jnp.argsort(group_id, stable=True)
    counts = jnp.zeros(GROUP_DEVS * EXPERTS, jnp.int32).at[group_id].add(1)
    starts = jnp.cumsum(counts) - counts
    sorted_rank = jnp.arange(TOKENS * TOP) - starts[group_id[sort_order]]
    slot_rank = jnp.zeros(TOKENS * TOP, jnp.int32).at[sort_order].set(sorted_rank.astype(jnp.int32))
    slot_idx = jnp.where(slot_rank < CAP, slot_rank, -1).reshape(TOKENS, TOP)
    return slot_idx.astype(jnp.int32), expert_ids.astype(jnp.int32)


def setup_inputs(seed: int = 0, part: int = 0) -> dict:
    base_key = jax.random.key(seed)
    key_wg, key_wu, key_wd = jax.random.split(base_key, 3)
    part_key = jax.random.fold_in(base_key, part)
    key_x, key_route, key_gate = jax.random.split(part_key, 3)
    x_disp = jax.random.normal(key_x, (GROUP_DEVS, EXPERTS, CAP, D), jnp.float32).astype(jnp.bfloat16)
    w_gate = (jax.random.normal(key_wg, (EXPERTS, D, FF), jnp.float32) * D ** -0.5).astype(jnp.bfloat16)
    w_up = (jax.random.normal(key_wu, (EXPERTS, D, FF), jnp.float32) * D ** -0.5).astype(jnp.bfloat16)
    w_down = (jax.random.normal(key_wd, (EXPERTS, FF, D), jnp.float32) * FF ** -0.5).astype(jnp.bfloat16)
    slot_idx, expert_ids = draw_routing(key_route)
    gate_wts = jax.nn.softmax(1.5 * jax.random.normal(key_gate, (TOKENS, TOP), jnp.float32), axis=1)
    return {"x_disp": x_disp, "w_gate": w_gate, "w_up": w_up, "w_down": w_down, "slot_idx": slot_idx, "expert_ids": expert_ids, "gate_wts": gate_wts}


def expert_ffn(expert_args):
    rows_e, gate_e, up_e, down_e = expert_args
    gate_proj = jnp.dot(rows_e, gate_e, preferred_element_type=jnp.float32)
    up_proj = jnp.dot(rows_e, up_e, preferred_element_type=jnp.float32)
    hidden = (jax.nn.silu(gate_proj) * up_proj).astype(jnp.bfloat16)
    return jnp.dot(hidden, down_e, preferred_element_type=jnp.float32).astype(jnp.bfloat16)


def reference(x_disp, w_gate, w_up, w_down, slot_idx, expert_ids, gate_wts):
    x_rows = jnp.transpose(x_disp, (1, 0, 2, 3)).reshape(EXPERTS, GROUP_DEVS * CAP, D)
    y_out = lax.map(expert_ffn, (x_rows, w_gate, w_up, w_down))
    y_flat = y_out.reshape(EXPERTS * GROUP_DEVS * CAP, D)
    source = jnp.arange(TOKENS) // TOK
    kept_mask = slot_idx >= 0
    flat_idx = jnp.where(kept_mask, (expert_ids * GROUP_DEVS + source[:, None]) * CAP + slot_idx, 0)
    weight = jnp.where(kept_mask, gate_wts, 0.0)

    def combine(source_args):
        pick_idx, pick_wts = source_args
        picked = jnp.take(y_flat, pick_idx, axis=0).astype(jnp.float32)
        return jnp.sum(picked * pick_wts[:, :, None], axis=1).astype(jnp.bfloat16)

    combined = lax.map(combine, (flat_idx.reshape(GROUP_DEVS, TOK, TOP), weight.reshape(GROUP_DEVS, TOK, TOP)))
    return combined.reshape(TOKENS, D)
```

```python
import functools

import jax
import jax.numpy as jnp
from jax import lax
from jax.experimental import pallas as pl
from jax.experimental.pallas import tpu as pltpu
from jax.sharding import PartitionSpec as P

MESH = pl.DeviceIdType.MESH
F32 = jnp.float32
BF16 = jnp.bfloat16
SLOTS = 3
BF16_MAX = 3.3895313892515355e38


def split_columns(width):
    return width // 2, 3 * width // 4


def kernel(outer, inner, x_hbm, wg_hbm, wu_hbm, wd_hbm, slot_ref, ids_ref, gate_ref, out_ref,
           x_buf, wg_buf, wu_buf, wd_buf, h_buf, y_send, y_in, y_out, route_tmp, route_send, route, pick, used,
           part_own, part_send, part_recv, out_buf,
           w_sem, route_ssem, route_rsem, a_ssem, a_rsem, b_ssem, b_rsem, c_ssem, c_rsem, p_ssem, p_rsem, out_sem):
    src, local, cap, width = x_hbm.shape
    tokens, top = slot_ref.shape
    ff = wg_hbm.shape[2]
    rows = src * cap
    span = local * cap
    block = inner * span
    cut_a, cut_b = split_columns(width)
    piece = 256 if width >= 2048 else 128
    o = lax.axis_index("outer")
    i = lax.axis_index("expert")

    def inner_peer(r):
        return lax.rem(i + r, inner)

    def outer_peer(r):
        return lax.rem(o + r, outer)

    def weight_copies(e, slot):
        return (
            pltpu.make_async_copy(x_hbm.at[:, e], x_buf.at[slot], w_sem.at[0, slot]),
            pltpu.make_async_copy(wg_hbm.at[e], wg_buf.at[slot], w_sem.at[1, slot]),
            pltpu.make_async_copy(wu_hbm.at[e], wu_buf.at[slot], w_sem.at[2, slot]),
            pltpu.make_async_copy(wd_hbm.at[e], wd_buf.at[slot], w_sem.at[3, slot]),
        )

    def inner_copy(e, r, lo, hi, ssem, rsem):
        return pltpu.make_async_remote_copy(
            src_ref=y_send.at[e, :, inner_peer(r), :, pl.ds(lo, hi - lo)],
            dst_ref=y_in.at[:, i, e, :, pl.ds(lo, hi - lo)],
            send_sem=ssem.at[e, r - 1], recv_sem=rsem.at[e, r - 1],
            device_id={"expert": inner_peer(r)}, device_id_type=MESH)

    def copy_a(e, r):
        return inner_copy(e, r, 0, cut_a, a_ssem, a_rsem)

    def copy_b(e, r):
        return inner_copy(e, r, cut_a, cut_b, b_ssem, b_rsem)

    def copy_c(e, r):
        return pltpu.make_async_remote_copy(
            src_ref=y_send.at[e, outer_peer(r), :, :, pl.ds(cut_b, width - cut_b)],
            dst_ref=y_out.at[:, o, e],
            send_sem=c_ssem.at[e, r - 1], recv_sem=c_rsem.at[e, r - 1],
            device_id={"outer": outer_peer(r)}, device_id_type=MESH)

    def copy_part(p, r):
        peer = {"outer": outer_peer(r)} if p * piece < cut_b else {"expert": inner_peer(r)}
        return pltpu.make_async_remote_copy(
            src_ref=part_send.at[r - 1, p], dst_ref=part_recv.at[r - 1, p],
            send_sem=p_ssem.at[r - 1, p], recv_sem=p_rsem.at[r - 1, p],
            device_id=peer, device_id_type=MESH)

    def copy_route(q):
        if q < outer - 1:
            r = q + 1
            dst, peer = route.at[o], {"outer": outer_peer(r)}
        else:
            r = q - (outer - 1) + 1
            dst, peer = route.at[outer + i], {"expert": inner_peer(r)}
        return pltpu.make_async_remote_copy(
            src_ref=route_send, dst_ref=dst, send_sem=route_ssem.at[q], recv_sem=route_rsem.at[q],
            device_id=peer, device_id_type=MESH)

    peers = outer + inner - 2
    barrier = pltpu.get_barrier_semaphore()
    for r in range(1, outer):
        pl.semaphore_signal(barrier, inc=1, device_id={"outer": outer_peer(r)}, device_id_type=MESH)
    for r in range(1, inner):
        pl.semaphore_signal(barrier, inc=1, device_id={"expert": inner_peer(r)}, device_id_type=MESH)
    for s in range(SLOTS):
        for c in weight_copies(s, s):
            c.start()

    slot = slot_ref[...]
    flat = jnp.where(slot >= 0, ids_ref[...] * cap + slot, -1).astype(F32)
    route_tmp[...] = jnp.zeros_like(route_tmp)
    route_tmp[:, 0:top] = flat
    route_tmp[:, top:2 * top] = gate_ref[...]
    lanes = route_tmp[...].T[0:2 * top]
    route_send[...] = lanes
    route[o] = lanes
    route[outer + i] = lanes
    pl.semaphore_wait(barrier, peers)
    for q in range(peers):
        copy_route(q).start()
    for q in range(peers):
        copy_route(q).wait_recv()

    row = lax.broadcasted_iota(jnp.int32, (block, tokens), 0)
    row_in = o * block + row
    row_out = (row // span) * block + i * span + row % span

    def build_pick(k):
        want = jnp.where(k < outer, row_in, row_out).astype(F32)
        gates = jnp.zeros((block, tokens), F32)
        hits = jnp.zeros((block, tokens), F32)
        for j in range(top):
            hit = want == route[k, j:j + 1, :]
            gates = jnp.where(hit, route[k, top + j:top + j + 1, :], gates)
            hits = jnp.where(hit, 1.0, hits)
        used[k] = jnp.broadcast_to(jnp.max(hits, axis=1, keepdims=True), (block, tokens)).astype(BF16)
        g = gates.T
        high = jnp.minimum(g, BF16_MAX).astype(BF16)
        rest = g - high.astype(F32)
        mid = rest.astype(BF16)
        low = (rest - mid.astype(F32)).astype(BF16)
        pick[k, 0:tokens] = high
        pick[k, tokens:2 * tokens] = mid
        pick[k, 2 * tokens:3 * tokens] = low

    def expert_step(e, carry):
        s = lax.rem(e, SLOTS)
        copies = weight_copies(e, s)
        build_pick(e)
        copies[0].wait()
        copies[1].wait()
        copies[2].wait()
        x = x_buf[s].reshape(rows, width)
        tile = 256
        for n in range(ff // tile):
            cols = pl.ds(n * tile, tile)
            gate = jnp.dot(x, wg_buf[s, :, cols], preferred_element_type=F32)
            up = jnp.dot(x, wu_buf[s, :, cols], preferred_element_type=F32)
            h_buf[:, cols] = (gate * lax.logistic(gate) * up).astype(BF16)
        copies[3].wait()
        h = h_buf[...]
        for n in range(width // tile):
            cols = pl.ds(n * tile, tile)
            y = jnp.dot(h, wd_buf[s, :, cols], preferred_element_type=F32).astype(BF16)
            y_send[e, :, :, :, cols] = y.reshape(outer, inner, cap, tile)
        y_in[:, i, e] = y_send[e, :, i, :, 0:cut_b]
        y_out[:, o, e] = y_send[e, o, :, :, cut_b:]

        @pl.when(e + SLOTS < local)
        def _():
            for c in weight_copies(e + SLOTS, s):
                c.start()

        for r in range(1, inner):
            copy_a(e, r).start()
        for r in range(1, outer):
            copy_c(e, r).start()
        return carry

    lax.fori_loop(0, local, expert_step, 0)

    def start_b(e, carry):
        for r in range(1, inner):
            copy_b(e, r).start()
        return carry

    lax.fori_loop(0, local, start_b, 0)

    def partial_sum(k, y):
        mask = jnp.concatenate([used[k]] * (piece // tokens), axis=1) > 0
        y = jnp.where(mask, y.reshape(block, piece), jnp.zeros((), BF16))
        s = jnp.dot(pick[k], y, preferred_element_type=F32)
        return s[0:tokens] + s[tokens:2 * tokens] + s[2 * tokens:3 * tokens]

    def combine(p):
        cols = pl.ds(p * piece, piece)
        over_outer = p * piece < cut_b
        n = outer if over_outer else inner
        for r in list(range(1, n)) + [0]:
            if over_outer:
                k = outer_peer(r)
                y = y_in[k, :, :, :, cols]
                total = partial_sum(k, y)
            else:
                k = inner_peer(r)
                y = y_out[k, :, :, :, pl.ds(p * piece - cut_b, piece)]
                total = partial_sum(outer + k, y)
            if r == 0:
                part_own[:, cols] = total
            else:
                part_send[r - 1, p] = total.astype(BF16)
                copy_part(p, r).start()

    def wait_all(copy, n):
        def body(e, carry):
            for r in range(1, n):
                copy(e, r).wait_recv()
            return carry
        lax.fori_loop(0, local, body, 0)

    pieces_a = range(0, cut_a // piece)
    pieces_b = range(cut_a // piece, cut_b // piece)
    pieces_c = range(cut_b // piece, width // piece)
    wait_all(copy_a, inner)
    for p in pieces_a:
        combine(p)
    wait_all(copy_c, outer)
    for p in pieces_c:
        combine(p)
    wait_all(copy_b, inner)
    for p in pieces_b:
        combine(p)

    for p in list(pieces_a) + list(pieces_c) + list(pieces_b):
        cols = pl.ds(p * piece, piece)
        n = outer if p * piece < cut_b else inner
        total = part_own[:, cols]
        for r in range(1, n):
            copy_part(p, r).wait_recv()
            total = total + part_recv[r - 1, p].astype(F32)
        out_buf[:, cols] = total.astype(BF16)

    write = pltpu.make_async_copy(out_buf, out_ref, out_sem)
    write.start()

    for q in range(peers):
        copy_route(q).wait_send()

    def drain(e, carry):
        for r in range(1, inner):
            copy_a(e, r).wait_send()
            copy_b(e, r).wait_send()
        for r in range(1, outer):
            copy_c(e, r).wait_send()
        return carry

    lax.fori_loop(0, local, drain, 0)
    for p in range(width // piece):
        n = outer if p * piece < cut_b else inner
        for r in range(1, n):
            copy_part(p, r).wait_send()
    write.wait()


def solution(mesh):
    outer = mesh.shape["outer"]
    inner = mesh.shape["expert"]

    def local_step(x_disp, w_gate, w_up, w_down, slot_idx, expert_ids, gate_wts):
        src, local, cap, width = x_disp.shape
        tokens, top = slot_idx.shape
        ff = w_gate.shape[2]
        block = inner * local * cap
        sources = outer + inner
        _, cut_b = split_columns(width)
        piece = 256 if width >= 2048 else 128
        dma = pltpu.SemaphoreType.DMA
        anywhere = pl.BlockSpec(memory_space=pl.ANY)
        vmem = pl.BlockSpec(memory_space=pltpu.VMEM)
        return pl.pallas_call(
            functools.partial(kernel, outer, inner),
            out_shape=jax.ShapeDtypeStruct((tokens, width), BF16),
            in_specs=[anywhere] * 4 + [vmem] * 3,
            out_specs=anywhere,
            scratch_shapes=[
                pltpu.VMEM((SLOTS, src, cap, width), BF16),
                pltpu.VMEM((SLOTS, width, ff), BF16),
                pltpu.VMEM((SLOTS, width, ff), BF16),
                pltpu.VMEM((SLOTS, ff, width), BF16),
                pltpu.VMEM((src * cap, ff), BF16),
                pltpu.VMEM((local, outer, inner, cap, width), BF16),
                pltpu.VMEM((outer, inner, local, cap, cut_b), BF16),
                pltpu.VMEM((inner, outer, local, cap, width - cut_b), BF16),
                pltpu.VMEM((tokens, 128), F32),
                pltpu.VMEM((2 * top, tokens), F32),
                pltpu.VMEM((sources, 2 * top, tokens), F32),
                pltpu.VMEM((sources, 3 * tokens, block), BF16),
                pltpu.VMEM((sources, block, tokens), BF16),
                pltpu.VMEM((tokens, width), F32),
                pltpu.VMEM((max(outer, inner) - 1, width // piece, tokens, piece), BF16),
                pltpu.VMEM((max(outer, inner) - 1, width // piece, tokens, piece), BF16),
                pltpu.VMEM((tokens, width), BF16),
                dma((4, SLOTS)),
                dma((outer + inner - 2,)), dma((outer + inner - 2,)),
                dma((local, inner - 1)), dma((local, inner - 1)),
                dma((local, inner - 1)), dma((local, inner - 1)),
                dma((local, outer - 1)), dma((local, outer - 1)),
                dma((max(outer, inner) - 1, width // piece)), dma((max(outer, inner) - 1, width // piece)),
                dma,
            ],
            compiler_params=pltpu.CompilerParams(
                collective_id=0, has_side_effects=True, vmem_limit_bytes=64_000_000),
        )(x_disp, w_gate, w_up, w_down, slot_idx, expert_ids, gate_wts)

    expert_spec = P(("outer", "expert"))
    token_spec = P(("data", "outer", "expert"))
    return jax.shard_map(local_step, mesh=mesh, in_specs=(P("data", ("outer", "expert")), expert_spec, expert_spec, expert_spec, token_spec, token_spec, token_spec), out_specs=token_spec, check_vma=False)
```

```python
import functools

import jax
import jax.numpy as jnp
from jax import lax
from jax.experimental import pallas as pl
from jax.experimental.pallas import tpu as pltpu
from jax.sharding import PartitionSpec as P

MESH = pl.DeviceIdType.MESH
F32 = jnp.float32
BF16 = jnp.bfloat16
SLOTS = 3
WINDOW = 4
BF16_MAX = 3.3895313892515355e38


def split_columns(width):
    return width // 2, 3 * width // 4


def kernel(outer, inner, x_hbm, wg_hbm, wu_hbm, wd_hbm, slot_ref, ids_ref, gate_ref, out_ref,
           x_buf, wg_buf, wu_buf, wd_buf, h_buf, y_send, y_in, y_out, route_send, route, pick, used,
           own, far, z_send, z_recv, c_send, c_recv, out_buf,
           w_sem, route_ssem, route_rsem, a_ssem, a_rsem, b_ssem, b_rsem, r_ssem, r_rsem,
           z_ssem, z_rsem, c_ssem, c_rsem, out_sem):
    src, local, cap, width = x_hbm.shape
    top, tokens = slot_ref.shape
    ff = wg_hbm.shape[2]
    rows = src * cap
    span = local * cap
    block = inner * span
    cut_a, cut_b = split_columns(width)
    piece = 256 if width >= 2048 else 128
    o = lax.axis_index("outer")
    i = lax.axis_index("expert")
    middle = lax.rem((o + 1) // 2, 2)
    half = o // 2
    near = o + 1 - 2 * lax.rem(o, 2)
    across = (2 - half, 3 - 3 * half)

    def inner_peer(r):
        return lax.rem(i + r, inner)

    def outer_peer(r):
        return lax.rem(o + r, outer)

    def weight_copy(e, kind):
        s = lax.rem(e, SLOTS)
        hbm, buf = ((wg_hbm, wg_buf), (wu_hbm, wu_buf), (wd_hbm, wd_buf))[kind]
        return pltpu.make_async_copy(hbm.at[e], buf.at[s], w_sem.at[kind, s])

    def x_copy(e):
        s = lax.rem(e, SLOTS)
        return pltpu.make_async_copy(x_hbm.at[:, e], x_buf.at[s], w_sem.at[3, s])

    def fetch(e, kind):
        @pl.when(e < local)
        def _():
            if kind == 0:
                x_copy(e).start()
            weight_copy(e, kind).start()

    def inner_copy(e, r, lo, hi, ssem, rsem):
        return pltpu.make_async_remote_copy(
            src_ref=y_send.at[e, :, inner_peer(r), :, pl.ds(lo, hi - lo)],
            dst_ref=y_in.at[:, i, e, :, pl.ds(lo, hi - lo)],
            send_sem=ssem.at[e, r - 1], recv_sem=rsem.at[e, r - 1],
            device_id={"expert": inner_peer(r)}, device_id_type=MESH)

    def copy_a(e, r):
        return inner_copy(e, r, 0, cut_a, a_ssem, a_rsem)

    def copy_b(e, r):
        return inner_copy(e, r, cut_a, cut_b, b_ssem, b_rsem)

    def copy_r(e, r):
        return pltpu.make_async_remote_copy(
            src_ref=y_send.at[e, outer_peer(r), :, :, pl.ds(cut_b, width - cut_b)],
            dst_ref=y_out.at[:, o, e],
            send_sem=r_ssem.at[e, r - 1], recv_sem=r_rsem.at[e, r - 1],
            device_id={"outer": outer_peer(r)}, device_id_type=MESH)

    def copy_z(p, q, slot, peer):
        return pltpu.make_async_remote_copy(
            src_ref=z_send.at[q, p], dst_ref=z_recv.at[slot, p],
            send_sem=z_ssem.at[q, p], recv_sem=z_rsem.at[slot, p],
            device_id={"outer": peer}, device_id_type=MESH)

    def copy_near(p):
        return copy_z(p, 0, 0, near)

    def copy_across(p, k):
        return copy_z(p, 1 + k, middle + (1 - middle) * (2 + k), middle * across[k] + (1 - middle) * near)

    def copy_c(p, r):
        return pltpu.make_async_remote_copy(
            src_ref=c_send.at[r - 1, p], dst_ref=c_recv.at[r - 1, p],
            send_sem=c_ssem.at[r - 1, p], recv_sem=c_rsem.at[r - 1, p],
            device_id={"expert": inner_peer(r)}, device_id_type=MESH)

    def copy_route(q):
        if q < outer - 1:
            r = q + 1
            dst, peer = route.at[o], {"outer": outer_peer(r)}
        else:
            r = q - (outer - 1) + 1
            dst, peer = route.at[outer + i], {"expert": inner_peer(r)}
        return pltpu.make_async_remote_copy(
            src_ref=route_send, dst_ref=dst, send_sem=route_ssem.at[q], recv_sem=route_rsem.at[q],
            device_id=peer, device_id_type=MESH)

    peers = outer + inner - 2
    barrier = pltpu.get_barrier_semaphore()
    for r in range(1, outer):
        pl.semaphore_signal(barrier, inc=1, device_id={"outer": outer_peer(r)}, device_id_type=MESH)
    for r in range(1, inner):
        pl.semaphore_signal(barrier, inc=1, device_id={"expert": inner_peer(r)}, device_id_type=MESH)
    for k in range(WINDOW):
        fetch(k // 3, k % 3)

    slot = slot_ref[...]
    flat = jnp.where(slot >= 0, ids_ref[...] * cap + slot, -1).astype(F32)
    lanes = jnp.concatenate([flat, gate_ref[...]], axis=0)
    route_send[...] = lanes
    route[o] = lanes
    route[outer + i] = lanes
    pl.semaphore_wait(barrier, peers)
    for q in range(peers):
        copy_route(q).start()

    row = lax.broadcasted_iota(jnp.int32, (block, tokens), 0)
    row_in = o * block + row
    row_out = (row // span) * block + i * span + row % span

    def build_pick(k):
        want = jnp.where(k < outer, row_in, row_out).astype(F32)
        gates = jnp.zeros((block, tokens), F32)
        hits = jnp.zeros((block, tokens), F32)
        for j in range(top):
            hit = want == route[k, j:j + 1, :]
            gates = jnp.where(hit, route[k, top + j:top + j + 1, :], gates)
            hits = jnp.where(hit, 1.0, hits)
        used[k] = jnp.broadcast_to(jnp.max(hits, axis=1, keepdims=True), (block, tokens)).astype(BF16)
        g = gates.T
        high = jnp.minimum(g, BF16_MAX).astype(BF16)
        rest = g - high.astype(F32)
        mid = rest.astype(BF16)
        low = (rest - mid.astype(F32)).astype(BF16)
        pick[k, 0:tokens] = high
        pick[k, tokens:2 * tokens] = mid
        pick[k, 2 * tokens:3 * tokens] = low

    def arrived(e, kind):
        if kind == 0:
            x_copy(e).wait()
        weight_copy(e, kind).wait()
        fetch(e + (kind + WINDOW) // 3, (kind + WINDOW) % 3)

    def expert_step(e, carry):
        s = lax.rem(e, SLOTS)
        arrived(e, 0)
        arrived(e, 1)
        x = x_buf[s].reshape(rows, width)
        tile = 256
        for n in range(ff // tile):
            cols = pl.ds(n * tile, tile)
            gate = jnp.dot(x, wg_buf[s, :, cols], preferred_element_type=F32)
            up = jnp.dot(x, wu_buf[s, :, cols], preferred_element_type=F32)
            h_buf[:, cols] = (gate * lax.logistic(gate) * up).astype(BF16)
        arrived(e, 2)
        h = h_buf[...]
        for n in range(width // tile):
            cols = pl.ds(n * tile, tile)
            y = jnp.dot(h, wd_buf[s, :, cols], preferred_element_type=F32).astype(BF16)
            y_send[e, :, :, :, cols] = y.reshape(outer, inner, cap, tile)
        y_in[:, i, e] = y_send[e, :, i, :, 0:cut_b]
        y_out[:, o, e] = y_send[e, o, :, :, cut_b:]
        for r in range(1, inner):
            copy_a(e, r).start()
        for r in range(1, outer):
            copy_r(e, r).start()

        @pl.when(e == 0)
        def _():
            for q in range(peers):
                copy_route(q).wait_recv()

        build_pick(e)
        return carry

    lax.fori_loop(0, local, expert_step, 0)

    def start_b(e, carry):
        for r in range(1, inner):
            copy_b(e, r).start()
        return carry

    lax.fori_loop(0, local, start_b, 0)

    def partial_sum(k, y):
        mask = jnp.concatenate([used[k]] * (piece // tokens), axis=1) > 0
        y = jnp.where(mask, y.reshape(block, piece), jnp.zeros((), BF16))
        s = jnp.dot(pick[k], y, preferred_element_type=F32)
        return s[0:tokens] + s[tokens:2 * tokens] + s[2 * tokens:3 * tokens]

    def columns(p):
        return pl.ds(p * piece, piece)

    def block_sum(p, k):
        return partial_sum(k, y_in[k, :, :, :, columns(p)])

    def wait_all(copy, n):
        def body(e, carry):
            for r in range(1, n):
                copy(e, r).wait_recv()
            return carry
        lax.fori_loop(0, local, body, 0)

    def combine(pieces):
        for p in pieces:
            for k in (1, 0):
                total = block_sum(p, across[k])

                @pl.when(middle == 1)
                def _():
                    far[k, :, columns(p)] = total

                @pl.when(middle == 0)
                def _():
                    z_send[1 + k, p] = total.astype(BF16)
                    copy_across(p, k).start()
        for p in pieces:
            z_send[0, p] = block_sum(p, near).astype(BF16)
            copy_near(p).start()
            own[:, columns(p)] = block_sum(p, o)

    def pass_on(pieces):
        @pl.when(middle == 1)
        def _():
            for p in pieces:
                for k in (1, 0):
                    copy_z(p, 1 + k, 2 + k, near).wait_recv()
                    z_send[1 + k, p] = (far[k, :, columns(p)] + z_recv[2 + k, p].astype(F32)).astype(BF16)
                    copy_across(p, k).start()

    def finish(pieces):
        for p in pieces:
            copy_z(p, 0, 0, near).wait_recv()
            copy_z(p, 1, 1, near).wait_recv()
            out_buf[:, columns(p)] = (own[:, columns(p)] + z_recv[0, p].astype(F32) + z_recv[1, p].astype(F32)).astype(BF16)

    pieces_a = range(0, cut_a // piece)
    pieces_b = range(cut_a // piece, cut_b // piece)
    pieces_c = range((width - cut_b) // piece)
    wait_all(copy_a, inner)
    combine(pieces_a)
    wait_all(copy_r, outer)
    for p in pieces_c:
        for r in range(1, inner):
            k = inner_peer(r)
            c_send[r - 1, p] = partial_sum(outer + k, y_out[k, :, :, :, columns(p)]).astype(BF16)
            copy_c(p, r).start()
        own[:, pl.ds(cut_b + p * piece, piece)] = partial_sum(outer + i, y_out[i, :, :, :, columns(p)])
    pass_on(pieces_a)
    wait_all(copy_b, inner)
    combine(pieces_b)
    pass_on(pieces_b)
    finish(pieces_a)
    for p in pieces_c:
        cols = pl.ds(cut_b + p * piece, piece)
        total = own[:, cols]
        for r in range(1, inner):
            copy_c(p, r).wait_recv()
            total = total + c_recv[r - 1, p].astype(F32)
        out_buf[:, cols] = total.astype(BF16)
    finish(pieces_b)

    write = pltpu.make_async_copy(out_buf, out_ref, out_sem)
    write.start()

    for q in range(peers):
        copy_route(q).wait_send()

    def drain(e, carry):
        for r in range(1, inner):
            copy_a(e, r).wait_send()
            copy_b(e, r).wait_send()
        for r in range(1, outer):
            copy_r(e, r).wait_send()
        return carry

    lax.fori_loop(0, local, drain, 0)
    for p in range(cut_b // piece):
        copy_near(p).wait_send()
        for k in (1, 0):
            copy_across(p, k).wait_send()
    for p in pieces_c:
        for r in range(1, inner):
            copy_c(p, r).wait_send()
    write.wait()


def solution(mesh):
    outer = mesh.shape["outer"]
    inner = mesh.shape["expert"]

    def local_step(x_disp, w_gate, w_up, w_down, slot_idx, expert_ids, gate_wts):
        src, local, cap, width = x_disp.shape
        tokens, top = slot_idx.shape
        ff = w_gate.shape[2]
        block = inner * local * cap
        sources = outer + inner
        _, cut_b = split_columns(width)
        piece = 256 if width >= 2048 else 128
        dma = pltpu.SemaphoreType.DMA
        anywhere = pl.BlockSpec(memory_space=pl.ANY)
        vmem = pl.BlockSpec(memory_space=pltpu.VMEM)
        return pl.pallas_call(
            functools.partial(kernel, outer, inner),
            out_shape=jax.ShapeDtypeStruct((tokens, width), BF16),
            in_specs=[anywhere] * 4 + [vmem] * 3,
            out_specs=anywhere,
            scratch_shapes=[
                pltpu.VMEM((SLOTS, src, cap, width), BF16),
                pltpu.VMEM((SLOTS, width, ff), BF16),
                pltpu.VMEM((SLOTS, width, ff), BF16),
                pltpu.VMEM((SLOTS, ff, width), BF16),
                pltpu.VMEM((src * cap, ff), BF16),
                pltpu.VMEM((local, outer, inner, cap, width), BF16),
                pltpu.VMEM((outer, inner, local, cap, cut_b), BF16),
                pltpu.VMEM((inner, outer, local, cap, width - cut_b), BF16),
                pltpu.VMEM((2 * top, tokens), F32),
                pltpu.VMEM((sources, 2 * top, tokens), F32),
                pltpu.VMEM((sources, 3 * tokens, block), BF16),
                pltpu.VMEM((sources, block, tokens), BF16),
                pltpu.VMEM((tokens, width), F32),
                pltpu.VMEM((2, tokens, cut_b), F32),
                pltpu.VMEM((3, cut_b // piece, tokens, piece), BF16),
                pltpu.VMEM((4, cut_b // piece, tokens, piece), BF16),
                pltpu.VMEM((inner - 1, (width - cut_b) // piece, tokens, piece), BF16),
                pltpu.VMEM((inner - 1, (width - cut_b) // piece, tokens, piece), BF16),
                pltpu.VMEM((tokens, width), BF16),
                dma((4, SLOTS)),
                dma((outer + inner - 2,)), dma((outer + inner - 2,)),
                dma((local, inner - 1)), dma((local, inner - 1)),
                dma((local, inner - 1)), dma((local, inner - 1)),
                dma((local, outer - 1)), dma((local, outer - 1)),
                dma((3, cut_b // piece)), dma((4, cut_b // piece)),
                dma((inner - 1, (width - cut_b) // piece)), dma((inner - 1, (width - cut_b) // piece)),
                dma,
            ],
            compiler_params=pltpu.CompilerParams(
                collective_id=0, has_side_effects=True, vmem_limit_bytes=64_000_000),
        )(x_disp, w_gate, w_up, w_down, slot_idx.T, expert_ids.T, gate_wts.T)

    expert_spec = P(("outer", "expert"))
    token_spec = P(("data", "outer", "expert"))
    return jax.shard_map(local_step, mesh=mesh, in_specs=(P("data", ("outer", "expert")), expert_spec, expert_spec, expert_spec, token_spec, token_spec, token_spec), out_specs=token_spec, check_vma=False)
```

```python
import functools

import jax
import jax.numpy as jnp
from jax import lax
from jax.experimental import pallas as pl
from jax.experimental.pallas import tpu as pltpu
from jax.sharding import PartitionSpec as P

MESH = pl.DeviceIdType.MESH
F32 = jnp.float32
BF16 = jnp.bfloat16
SLOTS = 3
WINDOW = 4
BF16_MAX = 3.3895313892515355e38


def column_plan(width):
    unit = width // 8
    return unit, (0, 2 * unit, 4 * unit, 6 * unit)


def kernel(outer, inner, x_hbm, wg_hbm, wu_hbm, wd_hbm, slot_ref, ids_ref, gate_ref, out_ref,
           x_buf, wg_buf, wu_buf, wd_buf, h_buf, y_send, y_in, y_out, route_send, route, pick, used,
           own, far, z_send, z_recv, c_send, c_recv,
           w_sem, route_ssem, route_rsem, i_ssem, i_rsem, r_ssem, r_rsem, z_ssem, z_rsem, c_ssem, c_rsem):
    src, local, cap, width = x_hbm.shape
    top, tokens = slot_ref.shape
    ff = wg_hbm.shape[2]
    rows = src * cap
    span = local * cap
    block = inner * span
    piece, bounds = column_plan(width)
    chunks = len(bounds) - 1
    split = bounds[-1]
    o = lax.axis_index("outer")
    i = lax.axis_index("expert")
    middle = lax.rem((o + 1) // 2, 2)
    half = o // 2
    near = o + 1 - 2 * lax.rem(o, 2)
    across = (2 - half, 3 - 3 * half)

    def inner_peer(r):
        return lax.rem(i + r, inner)

    def outer_peer(r):
        return lax.rem(o + r, outer)

    def weight_copy(e, kind):
        s = lax.rem(e, SLOTS)
        hbm, buf = ((wg_hbm, wg_buf), (wu_hbm, wu_buf), (wd_hbm, wd_buf))[kind]
        return pltpu.make_async_copy(hbm.at[e], buf.at[s], w_sem.at[kind, s])

    def x_copy(e):
        s = lax.rem(e, SLOTS)
        return pltpu.make_async_copy(x_hbm.at[:, e], x_buf.at[s], w_sem.at[3, s])

    def fetch(e, kind):
        @pl.when(e < local)
        def _():
            if kind == 0:
                x_copy(e).start()
            weight_copy(e, kind).start()

    def arrived(e, kind):
        if kind == 0:
            x_copy(e).wait()
        weight_copy(e, kind).wait()
        fetch(e + (kind + WINDOW) // 3, (kind + WINDOW) % 3)

    def inner_copy(src_ref, dst_ref, n, r):
        return pltpu.make_async_remote_copy(
            src_ref=src_ref, dst_ref=dst_ref, send_sem=i_ssem.at[n, r - 1], recv_sem=i_rsem.at[n, r - 1],
            device_id={"expert": inner_peer(r)}, device_id_type=MESH)

    def chunk_cols(n):
        return pl.ds(bounds[n], bounds[n + 1] - bounds[n])

    def send_inner(e, n):
        for r in range(1, inner):
            inner_copy(y_send.at[e, :, inner_peer(r), :, chunk_cols(n)], y_in.at[:, i, e, :, chunk_cols(n)], n, r).start()

    def all_inner(n, r):
        return inner_copy(y_send.at[:, :, inner_peer(r), :, chunk_cols(n)],
                          y_in.at[:, lax.rem(i + inner - r, inner), :, :, chunk_cols(n)], n, r)

    def outer_copy(src_ref, dst_ref, r):
        return pltpu.make_async_remote_copy(
            src_ref=src_ref, dst_ref=dst_ref, send_sem=r_ssem.at[r - 1], recv_sem=r_rsem.at[r - 1],
            device_id={"outer": outer_peer(r)}, device_id_type=MESH)

    rest_cols = pl.ds(split, width - split)

    def send_outer(e):
        for r in range(1, outer):
            outer_copy(y_send.at[e, outer_peer(r), :, :, rest_cols], y_out.at[:, o, e], r).start()

    def all_outer(r):
        return outer_copy(y_send.at[:, outer_peer(r), :, :, rest_cols], y_out.at[:, lax.rem(o + outer - r, outer)], r)

    def copy_z(p, q, slot, peer):
        return pltpu.make_async_remote_copy(
            src_ref=z_send.at[q, p], dst_ref=z_recv.at[slot, p],
            send_sem=z_ssem.at[q, p], recv_sem=z_rsem.at[slot, p],
            device_id={"outer": peer}, device_id_type=MESH)

    def copy_near(p):
        return copy_z(p, 0, 0, near)

    def copy_across(p, k):
        return copy_z(p, 1 + k, middle + (1 - middle) * (2 + k), middle * across[k] + (1 - middle) * near)

    def copy_c(p, r):
        return pltpu.make_async_remote_copy(
            src_ref=c_send.at[r - 1, p], dst_ref=c_recv.at[r - 1, p],
            send_sem=c_ssem.at[r - 1, p], recv_sem=c_rsem.at[r - 1, p],
            device_id={"expert": inner_peer(r)}, device_id_type=MESH)

    def copy_route(q):
        if q < outer - 1:
            dst, peer = route.at[o], {"outer": outer_peer(q + 1)}
        else:
            dst, peer = route.at[outer + i], {"expert": inner_peer(q - outer + 2)}
        return pltpu.make_async_remote_copy(
            src_ref=route_send, dst_ref=dst, send_sem=route_ssem.at[q], recv_sem=route_rsem.at[q],
            device_id=peer, device_id_type=MESH)

    for k in range(WINDOW):
        fetch(k // 3, k % 3)
    peers = outer + inner - 2
    barrier = pltpu.get_barrier_semaphore()
    for r in range(1, outer):
        pl.semaphore_signal(barrier, inc=1, device_id={"outer": outer_peer(r)}, device_id_type=MESH)
    for r in range(1, inner):
        pl.semaphore_signal(barrier, inc=1, device_id={"expert": inner_peer(r)}, device_id_type=MESH)

    slot = slot_ref[...]
    flat = jnp.where(slot >= 0, ids_ref[...] * cap + slot, -1).astype(F32)
    lanes = jnp.concatenate([flat, gate_ref[...]], axis=0)
    route_send[...] = lanes
    route[o] = lanes
    route[outer + i] = lanes
    pl.semaphore_wait(barrier, peers)
    for q in range(peers):
        copy_route(q).start()

    row = lax.broadcasted_iota(jnp.int32, (block, tokens), 0)
    row_in = o * block + row
    row_out = (row // span) * block + i * span + row % span

    def build_pick(k):
        want = jnp.where(k < outer, row_in, row_out).astype(F32)
        gates = jnp.zeros((block, tokens), F32)
        hits = jnp.zeros((block, tokens), F32)
        for j in range(top):
            hit = want == route[k, j:j + 1, :]
            gates = jnp.where(hit, route[k, top + j:top + j + 1, :], gates)
            hits = jnp.where(hit, 1.0, hits)
        used[k] = jnp.broadcast_to(jnp.max(hits, axis=1, keepdims=True), (block, tokens)).astype(BF16)
        g = gates.T
        high = jnp.minimum(g, BF16_MAX).astype(BF16)
        rest = g - high.astype(F32)
        mid = rest.astype(BF16)
        low = (rest - mid.astype(F32)).astype(BF16)
        pick[k, 0:tokens] = high
        pick[k, tokens:2 * tokens] = mid
        pick[k, 2 * tokens:3 * tokens] = low

    def expert_step(e, carry):
        s = lax.rem(e, SLOTS)
        arrived(e, 0)
        arrived(e, 1)
        x = x_buf[s].reshape(rows, width)
        tile = 256
        for n in range(ff // tile):
            cols = pl.ds(n * tile, tile)
            gate = jnp.dot(x, wg_buf[s, :, cols], preferred_element_type=F32)
            up = jnp.dot(x, wu_buf[s, :, cols], preferred_element_type=F32)
            h_buf[:, cols] = (gate * lax.logistic(gate) * up).astype(BF16)
        arrived(e, 2)
        h = h_buf[...]

        def down(lo, hi):
            for c in range(lo, hi, piece):
                cols = pl.ds(c, piece)
                y = jnp.dot(h, wd_buf[s, :, cols], preferred_element_type=F32).astype(BF16)
                y_send[e, :, :, :, cols] = y.reshape(outer, inner, cap, piece)

        down(bounds[0], bounds[1])
        down(split, width)
        send_inner(e, 0)
        down(bounds[1], bounds[2])
        send_outer(e)
        down(bounds[2], split)
        send_inner(e, 1)
        y_in[:, i, e] = y_send[e, :, i, :, 0:split]
        y_out[:, o, e] = y_send[e, o, :, :, split:]

        @pl.when(e == 0)
        def _():
            for q in range(peers):
                copy_route(q).wait_recv()

        build_pick(e)
        return carry

    lax.fori_loop(0, local, expert_step, 0)

    def send_last(e, carry):
        send_inner(e, 2)
        return carry

    lax.fori_loop(0, local, send_last, 0)

    def partial_sum(k, y):
        mask = jnp.concatenate([used[k]] * (piece // tokens), axis=1) > 0
        y = jnp.where(mask, y.reshape(block, piece), jnp.zeros((), BF16))
        s = jnp.dot(pick[k], y, preferred_element_type=F32)
        return s[0:tokens] + s[tokens:2 * tokens] + s[2 * tokens:3 * tokens]

    def columns(p):
        return pl.ds(p * piece, piece)

    def block_sum(p, k):
        return partial_sum(k, y_in[k, :, :, :, columns(p)])

    def pieces_of(n):
        return range(bounds[n] // piece, bounds[n + 1] // piece)

    def combine(n):
        for r in range(1, inner):
            all_inner(n, r).wait_recv()
        for p in pieces_of(n):
            for k in (1, 0):
                total = block_sum(p, across[k])

                @pl.when(middle == 1)
                def _():
                    far[k, :, columns(p)] = total

                @pl.when(middle == 0)
                def _():
                    z_send[1 + k, p] = total.astype(BF16)
                    copy_across(p, k).start()
        for p in pieces_of(n):
            z_send[0, p] = block_sum(p, near).astype(BF16)
            copy_near(p).start()
        for p in pieces_of(n):
            own[:, columns(p)] = block_sum(p, o)

    def pass_on(n):
        @pl.when(middle == 1)
        def _():
            for p in pieces_of(n):
                for k in (1, 0):
                    copy_z(p, 1 + k, 2 + k, near).wait_recv()
                    z_send[1 + k, p] = (far[k, :, columns(p)] + z_recv[2 + k, p].astype(F32)).astype(BF16)
                    copy_across(p, k).start()

    def finish(n):
        for p in pieces_of(n):
            copy_z(p, 0, 0, near).wait_recv()
            copy_z(p, 1, 1, near).wait_recv()
            out_ref[:, columns(p)] = (own[:, columns(p)] + z_recv[0, p].astype(F32) + z_recv[1, p].astype(F32)).astype(BF16)

    rest_pieces = range((width - split) // piece)
    combine(0)
    combine(1)
    for r in range(1, outer):
        all_outer(r).wait_recv()
    for p in rest_pieces:
        for r in range(1, inner):
            k = inner_peer(r)
            c_send[r - 1, p] = partial_sum(outer + k, y_out[k, :, :, :, columns(p)]).astype(BF16)
            copy_c(p, r).start()
        own[:, pl.ds(split + p * piece, piece)] = partial_sum(outer + i, y_out[i, :, :, :, columns(p)])
    pass_on(0)
    pass_on(1)
    combine(2)
    pass_on(2)
    finish(0)
    finish(1)
    for p in rest_pieces:
        cols = pl.ds(split + p * piece, piece)
        total = own[:, cols]
        for r in range(1, inner):
            copy_c(p, r).wait_recv()
            total = total + c_recv[r - 1, p].astype(F32)
        out_ref[:, cols] = total.astype(BF16)

    for q in range(peers):
        copy_route(q).wait_send()
    for r in range(1, inner):
        for n in range(chunks):
            all_inner(n, r).wait_send()
        for p in rest_pieces:
            copy_c(p, r).wait_send()
    for r in range(1, outer):
        all_outer(r).wait_send()
    for p in range(split // piece):
        copy_near(p).wait_send()
        for k in (1, 0):
            copy_across(p, k).wait_send()
    finish(2)


def solution(mesh):
    outer = mesh.shape["outer"]
    inner = mesh.shape["expert"]

    def local_step(x_disp, w_gate, w_up, w_down, slot_idx, expert_ids, gate_wts):
        src, local, cap, width = x_disp.shape
        tokens, top = slot_idx.shape
        ff = w_gate.shape[2]
        block = inner * local * cap
        sources = outer + inner
        piece, bounds = column_plan(width)
        chunks = len(bounds) - 1
        split = bounds[-1]
        peers = outer + inner - 2
        dma = pltpu.SemaphoreType.DMA
        anywhere = pl.BlockSpec(memory_space=pl.ANY)
        vmem = pl.BlockSpec(memory_space=pltpu.VMEM)
        return pl.pallas_call(
            functools.partial(kernel, outer, inner),
            out_shape=jax.ShapeDtypeStruct((tokens, width), BF16),
            in_specs=[anywhere] * 4 + [vmem] * 3,
            out_specs=vmem,
            scratch_shapes=[
                pltpu.VMEM((SLOTS, src, cap, width), BF16),
                pltpu.VMEM((SLOTS, width, ff), BF16),
                pltpu.VMEM((SLOTS, width, ff), BF16),
                pltpu.VMEM((SLOTS, ff, width), BF16),
                pltpu.VMEM((src * cap, ff), BF16),
                pltpu.VMEM((local, outer, inner, cap, width), BF16),
                pltpu.VMEM((outer, inner, local, cap, split), BF16),
                pltpu.VMEM((inner, outer, local, cap, width - split), BF16),
                pltpu.VMEM((2 * top, tokens), F32),
                pltpu.VMEM((sources, 2 * top, tokens), F32),
                pltpu.VMEM((sources, 3 * tokens, block), BF16),
                pltpu.VMEM((sources, block, tokens), BF16),
                pltpu.VMEM((tokens, width), F32),
                pltpu.VMEM((2, tokens, split), F32),
                pltpu.VMEM((3, split // piece, tokens, piece), BF16),
                pltpu.VMEM((4, split // piece, tokens, piece), BF16),
                pltpu.VMEM((inner - 1, (width - split) // piece, tokens, piece), BF16),
                pltpu.VMEM((inner - 1, (width - split) // piece, tokens, piece), BF16),
                dma((4, SLOTS)),
                dma((peers,)), dma((peers,)),
                dma((chunks, inner - 1)), dma((chunks, inner - 1)),
                dma((outer - 1,)), dma((outer - 1,)),
                dma((3, split // piece)), dma((4, split // piece)),
                dma((inner - 1, (width - split) // piece)), dma((inner - 1, (width - split) // piece)),
            ],
            compiler_params=pltpu.CompilerParams(
                collective_id=0, has_side_effects=True, vmem_limit_bytes=54_000_000),
        )(x_disp, w_gate, w_up, w_down, slot_idx.T, expert_ids.T, gate_wts.T)

    expert_spec = P(("outer", "expert"))
    token_spec = P(("data", "outer", "expert"))
    return jax.shard_map(local_step, mesh=mesh, in_specs=(P("data", ("outer", "expert")), expert_spec, expert_spec, expert_spec, token_spec, token_spec, token_spec), out_specs=token_spec, check_vma=False)
```

```python
import functools

import jax
import jax.numpy as jnp
from jax import lax
from jax.experimental import pallas as pl
from jax.experimental.pallas import tpu as pltpu
from jax.sharding import PartitionSpec as P

MESH = pl.DeviceIdType.MESH
F32 = jnp.float32
BF16 = jnp.bfloat16
SLOTS = 3
WINDOW = 4
BF16_MAX = 3.3895313892515355e38


CHUNKS = 8
FIRST = (0, 1, 2)
LATER = 3
MIXED = (4, 5)
OUTER = (6, 7)
INNER_CHUNKS = 6


def kernel(outer, inner, x_hbm, wg_hbm, wu_hbm, wd_hbm, slot_hbm, ids_hbm, gate_hbm, out_ref,
           x_buf, wg_buf, wu_buf, wd_buf, h_buf, y_send, y_in, y_out, y_half, slot_ref, ids_ref, gate_ref, route_send, route, pick, used,
           own, far, z_send, z_recv, c_send, c_recv,
           w_sem, t_sem, route_ssem, route_rsem, i_ssem, i_rsem, r_ssem, r_rsem, h_ssem, h_rsem, z_ssem, z_rsem, c_ssem, c_rsem):
    src, local, cap, width = x_hbm.shape
    top, tokens = slot_hbm.shape
    ff = wg_hbm.shape[2]
    rows = src * cap
    span = local * cap
    block = inner * span
    piece = width // CHUNKS
    split = INNER_CHUNKS * piece
    mixed = MIXED[0] * piece
    o = lax.axis_index("outer")
    i = lax.axis_index("expert")
    middle = lax.rem((o + 1) // 2, 2)
    half = o // 2
    seat = lax.rem(o, 2)
    near = o + 1 - 2 * seat
    across = (2 - half, 3 - 3 * half)

    def inner_peer(r):
        return lax.rem(i + r, inner)

    def outer_peer(r):
        return lax.rem(o + r, outer)

    def weight_copy(e, kind):
        s = lax.rem(e, SLOTS)
        hbm, buf = ((wg_hbm, wg_buf), (wu_hbm, wu_buf), (wd_hbm, wd_buf))[kind]
        return pltpu.make_async_copy(hbm.at[e], buf.at[s], w_sem.at[kind, s])

    def x_copy(e):
        s = lax.rem(e, SLOTS)
        return pltpu.make_async_copy(x_hbm.at[:, e], x_buf.at[s], w_sem.at[3, s])

    def fetch(e, kind):
        @pl.when(e < local)
        def _():
            if kind == 0:
                x_copy(e).start()
            weight_copy(e, kind).start()

    def arrived(e, kind):
        if kind == 0:
            x_copy(e).wait()
        weight_copy(e, kind).wait()
        fetch(e + (kind + WINDOW) // 3, (kind + WINDOW) % 3)

    def inner_copy(src_ref, dst_ref, n, r):
        return pltpu.make_async_remote_copy(
            src_ref=src_ref, dst_ref=dst_ref, send_sem=i_ssem.at[n, r - 1], recv_sem=i_rsem.at[n, r - 1],
            device_id={"expert": inner_peer(r)}, device_id_type=MESH)

    def chunk_cols(n):
        return pl.ds(n * piece, piece)

    def blocks(n):
        return pl.ds(2 * (1 - half), 2) if n in MIXED else pl.ds(0, outer)

    def send_inner(e, n):
        for r in range(1, inner):
            inner_copy(y_send.at[e, blocks(n), inner_peer(r), :, chunk_cols(n)],
                       y_in.at[blocks(n), i, e, :, chunk_cols(n)], n, r).start()

    def all_inner(n, r):
        return inner_copy(y_send.at[:, blocks(n), inner_peer(r), :, chunk_cols(n)],
                          y_in.at[blocks(n), lax.rem(i + inner - r, inner), :, :, chunk_cols(n)], n, r)

    def outer_copy(src_ref, dst_ref, r):
        return pltpu.make_async_remote_copy(
            src_ref=src_ref, dst_ref=dst_ref, send_sem=r_ssem.at[r - 1], recv_sem=r_rsem.at[r - 1],
            device_id={"outer": outer_peer(r)}, device_id_type=MESH)

    rest_cols = pl.ds(split, width - split)

    def send_outer(e):
        for r in range(1, outer):
            outer_copy(y_send.at[e, outer_peer(r), :, :, rest_cols], y_out.at[:, o, e], r).start()

    def all_outer(r):
        return outer_copy(y_send.at[:, outer_peer(r), :, :, rest_cols], y_out.at[:, lax.rem(o + outer - r, outer)], r)

    half_cols = pl.ds(mixed, split - mixed)

    def half_copy(src_ref, dst_ref):
        return pltpu.make_async_remote_copy(
            src_ref=src_ref, dst_ref=dst_ref, send_sem=h_ssem, recv_sem=h_rsem,
            device_id={"outer": near}, device_id_type=MESH)

    def send_half(e):
        half_copy(y_send.at[e, near, :, :, half_cols], y_half.at[:, seat, e]).start()

    def all_half():
        return half_copy(y_send.at[:, near, :, :, half_cols], y_half.at[:, 1 - seat])

    def copy_z(p, q, slot, peer):
        return pltpu.make_async_remote_copy(
            src_ref=z_send.at[q, p], dst_ref=z_recv.at[slot, p],
            send_sem=z_ssem.at[q, p], recv_sem=z_rsem.at[slot, p],
            device_id={"outer": peer}, device_id_type=MESH)

    def copy_near(p):
        return copy_z(p, 0, 0, near)

    def copy_across(p, k):
        return copy_z(p, 1 + k, middle + (1 - middle) * (2 + k), middle * across[k] + (1 - middle) * near)

    def copy_c(p, r):
        return pltpu.make_async_remote_copy(
            src_ref=c_send.at[r - 1, p], dst_ref=c_recv.at[r - 1, p],
            send_sem=c_ssem.at[r - 1, p], recv_sem=c_rsem.at[r - 1, p],
            device_id={"expert": inner_peer(r)}, device_id_type=MESH)

    def copy_route(q):
        if q < outer - 1:
            dst, peer = route.at[o], {"outer": outer_peer(q + 1)}
        else:
            dst, peer = route.at[outer + i], {"expert": inner_peer(q - outer + 2)}
        return pltpu.make_async_remote_copy(
            src_ref=route_send, dst_ref=dst, send_sem=route_ssem.at[q], recv_sem=route_rsem.at[q],
            device_id=peer, device_id_type=MESH)

    small = [pltpu.make_async_copy(a, b, t_sem.at[k]) for k, (a, b) in enumerate(
        ((slot_hbm, slot_ref), (ids_hbm, ids_ref), (gate_hbm, gate_ref)))]
    for c in small:
        c.start()
    for k in range(WINDOW):
        fetch(k // 3, k % 3)
    peers = outer + inner - 2
    barrier = pltpu.get_barrier_semaphore()
    for r in range(1, outer):
        pl.semaphore_signal(barrier, inc=1, device_id={"outer": outer_peer(r)}, device_id_type=MESH)
    for r in range(1, inner):
        pl.semaphore_signal(barrier, inc=1, device_id={"expert": inner_peer(r)}, device_id_type=MESH)

    for c in small:
        c.wait()
    slot = slot_ref[...]
    flat = jnp.where(slot >= 0, ids_ref[...] * cap + slot, -1).astype(F32)
    lanes = jnp.concatenate([flat, gate_ref[...]], axis=0)
    route_send[...] = lanes
    route[o] = lanes
    route[outer + i] = lanes
    pl.semaphore_wait(barrier, peers)
    for q in range(peers):
        copy_route(q).start()

    row = lax.broadcasted_iota(jnp.int32, (block, tokens), 0)
    row_in = o * block + row
    row_out = (row // span) * block + i * span + row % span

    def build_pick(k):
        want = jnp.where(k < outer, row_in, row_out).astype(F32)
        gates = jnp.zeros((block, tokens), F32)
        hits = jnp.zeros((block, tokens), F32)
        for j in range(top):
            hit = want == route[k, j:j + 1, :]
            gates = jnp.where(hit, route[k, top + j:top + j + 1, :], gates)
            hits = jnp.where(hit, 1.0, hits)
        used[k] = jnp.broadcast_to(jnp.max(hits, axis=1, keepdims=True), (block, tokens)).astype(BF16)
        g = gates.T
        high = jnp.minimum(g, BF16_MAX).astype(BF16)
        rest = g - high.astype(F32)
        mid = rest.astype(BF16)
        low = (rest - mid.astype(F32)).astype(BF16)
        pick[k, 0:tokens] = high
        pick[k, tokens:2 * tokens] = mid
        pick[k, 2 * tokens:3 * tokens] = low

    def expert_step(e, carry):
        s = lax.rem(e, SLOTS)
        arrived(e, 0)
        arrived(e, 1)
        x = x_buf[s].reshape(rows, width)
        tile = 256
        for n in range(ff // tile):
            cols = pl.ds(n * tile, tile)
            gate = jnp.dot(x, wg_buf[s, :, cols], preferred_element_type=F32)
            up = jnp.dot(x, wu_buf[s, :, cols], preferred_element_type=F32)
            h_buf[:, cols] = (gate * lax.logistic(gate) * up).astype(BF16)
        arrived(e, 2)
        h = h_buf[...]

        def down(*numbers):
            for n in numbers:
                y = jnp.dot(h, wd_buf[s, :, chunk_cols(n)], preferred_element_type=F32).astype(BF16)
                y_send[e, :, :, :, chunk_cols(n)] = y.reshape(outer, inner, cap, piece)

        down(0, 1)
        send_inner(e, 0)
        down(2)
        send_inner(e, 1)
        down(6, 7)
        send_inner(e, 2)
        down(4)
        send_outer(e)
        down(5, 3)
        send_half(e)
        y_in[:, i, e] = y_send[e, :, i, :, 0:split]
        y_out[:, o, e] = y_send[e, o, :, :, split:]
        y_half[:, seat, e] = y_send[e, o, :, :, mixed:split]

        @pl.when(e == 0)
        def _():
            for q in range(peers):
                copy_route(q).wait_recv()

        build_pick(e)
        return carry

    lax.fori_loop(0, local, expert_step, 0)

    for n in (LATER,) + MIXED:
        def send_last(e, carry):
            send_inner(e, n)
            return carry

        lax.fori_loop(0, local, send_last, 0)

    def partial_sum(k, slots, y):
        mask = jnp.concatenate([used[k, slots]] * (piece // tokens), axis=1) > 0
        y = jnp.where(mask, y, jnp.zeros((), BF16))
        s = jnp.dot(pick[k, :, slots], y, preferred_element_type=F32)
        return s[0:tokens] + s[tokens:2 * tokens] + s[2 * tokens:3 * tokens]

    def block_sum(n, k):
        return partial_sum(k, pl.ds(0, block), y_in[k, :, :, :, chunk_cols(n)].reshape(block, piece))

    def half_sum(n, k):
        y = y_half[k, :, :, :, pl.ds(n * piece - mixed, piece)].reshape(2 * span, piece)
        return partial_sum(outer + k, pl.ds(pl.multiple_of(half * 2 * span, 2 * span), 2 * span), y)

    def outer_sum(n, k):
        y = y_out[k, :, :, :, pl.ds(n * piece - split, piece)].reshape(block, piece)
        return partial_sum(outer + k, pl.ds(0, block), y)

    def sum_across(n):
        for r in range(1, inner):
            all_inner(n, r).wait_recv()
        for k in (1, 0):
            total = block_sum(n, across[k])

            @pl.when(middle == 1)
            def _():
                far[k, :, chunk_cols(n)] = total

            @pl.when(middle == 0)
            def _():
                z_send[1 + k, n] = total.astype(BF16)
                copy_across(n, k).start()

    def sum_near(n):
        z_send[0, n] = block_sum(n, near).astype(BF16)
        copy_near(n).start()

    def sum_inner(n, of):
        for r in range(1, inner):
            c_send[r - 1, n - MIXED[0]] = of(n, inner_peer(r)).astype(BF16)
            copy_c(n - MIXED[0], r).start()
        own[:, chunk_cols(n)] = of(n, i)

    def pass_on(n):
        @pl.when(middle == 1)
        def _():
            for k in (1, 0):
                copy_z(n, 1 + k, 2 + k, near).wait_recv()
                z_send[1 + k, n] = (far[k, :, chunk_cols(n)] + z_recv[2 + k, n].astype(F32)).astype(BF16)
                copy_across(n, k).start()

    def finish(n):
        total = own[:, chunk_cols(n)]
        if n < MIXED[0]:
            copy_z(n, 0, 0, near).wait_recv()
            total = total + z_recv[0, n].astype(F32)
        else:
            for r in range(1, inner):
                copy_c(n - MIXED[0], r).wait_recv()
                total = total + c_recv[r - 1, n - MIXED[0]].astype(F32)
        if n < INNER_CHUNKS:
            copy_z(n, 1, 1, near).wait_recv()
            total = total + z_recv[1, n].astype(F32)
        out_ref[:, chunk_cols(n)] = total.astype(BF16)

    for n in FIRST:
        sum_across(n)
    for r in range(1, outer):
        all_outer(r).wait_recv()
    all_half().wait_recv()
    for n in OUTER:
        sum_inner(n, outer_sum)
    for n in MIXED:
        sum_inner(n, half_sum)
    pass_on(0)
    sum_across(3)
    pass_on(1)
    sum_across(4)
    pass_on(2)
    sum_across(5)
    for n in FIRST + (LATER,):
        sum_near(n)
    pass_on(3)
    for n in FIRST + (LATER,):
        own[:, chunk_cols(n)] = block_sum(n, o)
    pass_on(4)
    pass_on(5)

    for q in range(peers):
        copy_route(q).wait_send()
    for r in range(1, inner):
        for n in range(INNER_CHUNKS):
            all_inner(n, r).wait_send()
    for r in range(1, outer):
        all_outer(r).wait_send()
    all_half().wait_send()
    for n in OUTER + MIXED:
        finish(n)
    for n in FIRST + (LATER,):
        finish(n)
    for n in OUTER + MIXED:
        for r in range(1, inner):
            copy_c(n - MIXED[0], r).wait_send()
    for n in range(INNER_CHUNKS):
        if n < MIXED[0]:
            copy_near(n).wait_send()
        for k in (1, 0):
            copy_across(n, k).wait_send()


def solution(mesh):
    outer = mesh.shape["outer"]
    inner = mesh.shape["expert"]

    def local_step(x_disp, w_gate, w_up, w_down, slot_idx, expert_ids, gate_wts):
        src, local, cap, width = x_disp.shape
        tokens, top = slot_idx.shape
        ff = w_gate.shape[2]
        block = inner * local * cap
        sources = outer + inner
        piece = width // CHUNKS
        split = INNER_CHUNKS * piece
        turned = CHUNKS - MIXED[0]
        peers = outer + inner - 2
        dma = pltpu.SemaphoreType.DMA
        hbm = pl.BlockSpec(memory_space=pltpu.HBM)
        vmem = pl.BlockSpec(memory_space=pltpu.VMEM)
        return pl.pallas_call(
            functools.partial(kernel, outer, inner),
            out_shape=jax.ShapeDtypeStruct((tokens, width), BF16),
            in_specs=[hbm] * 7,
            out_specs=vmem,
            scratch_shapes=[
                pltpu.VMEM((SLOTS, src, cap, width), BF16),
                pltpu.VMEM((SLOTS, width, ff), BF16),
                pltpu.VMEM((SLOTS, width, ff), BF16),
                pltpu.VMEM((SLOTS, ff, width), BF16),
                pltpu.VMEM((src * cap, ff), BF16),
                pltpu.VMEM((local, outer, inner, cap, width), BF16),
                pltpu.VMEM((outer, inner, local, cap, split), BF16),
                pltpu.VMEM((inner, outer, local, cap, width - split), BF16),
                pltpu.VMEM((inner, 2, local, cap, len(MIXED) * piece), BF16),
                pltpu.VMEM((top, tokens), jnp.int32),
                pltpu.VMEM((top, tokens), jnp.int32),
                pltpu.VMEM((top, tokens), F32),
                pltpu.VMEM((2 * top, tokens), F32),
                pltpu.VMEM((sources, 2 * top, tokens), F32),
                pltpu.VMEM((sources, 3 * tokens, block), BF16),
                pltpu.VMEM((sources, block, tokens), BF16),
                pltpu.VMEM((tokens, width), F32),
                pltpu.VMEM((2, tokens, split), F32),
                pltpu.VMEM((3, INNER_CHUNKS, tokens, piece), BF16),
                pltpu.VMEM((4, INNER_CHUNKS, tokens, piece), BF16),
                pltpu.VMEM((inner - 1, turned, tokens, piece), BF16),
                pltpu.VMEM((inner - 1, turned, tokens, piece), BF16),
                dma((4, SLOTS)), dma((3,)),
                dma((peers,)), dma((peers,)),
                dma((INNER_CHUNKS, inner - 1)), dma((INNER_CHUNKS, inner - 1)),
                dma((outer - 1,)), dma((outer - 1,)),
                dma, dma,
                dma((3, INNER_CHUNKS)), dma((4, INNER_CHUNKS)),
                dma((inner - 1, turned)), dma((inner - 1, turned)),
            ],
            compiler_params=pltpu.CompilerParams(
                collective_id=0, has_side_effects=True, vmem_limit_bytes=54_000_000),
        )(x_disp, w_gate, w_up, w_down, slot_idx.T, expert_ids.T, gate_wts.T)

    expert_spec = P(("outer", "expert"))
    token_spec = P(("data", "outer", "expert"))
    return jax.shard_map(local_step, mesh=mesh, in_specs=(P("data", ("outer", "expert")), expert_spec, expert_spec, expert_spec, token_spec, token_spec, token_spec), out_specs=token_spec, check_vma=False)
```

```python
import functools

import jax
import jax.numpy as jnp
from jax import lax
from jax.experimental import pallas as pl
from jax.experimental.pallas import tpu as pltpu
from jax.sharding import PartitionSpec as P

MESH = pl.DeviceIdType.MESH
F32 = jnp.float32
BF16 = jnp.bfloat16
SLOTS = 3
WINDOW = 4
BF16_MAX = 3.3895313892515355e38


CHUNKS = 8
FIRST = (0, 1, 2)
LATER = 3
MIXED = (4, 5)
OUTER = (6, 7)
INNER_CHUNKS = 6


def kernel(outer, inner, x_hbm, wg_hbm, wu_hbm, wd_hbm, slot_hbm, ids_hbm, gate_hbm, out_ref,
           x_buf, wg_buf, wu_buf, wd_buf, h_buf, in_send, out_send, half_send, y_in, y_out, y_half, slot_ref, ids_ref, gate_ref, route_send, route, pick, used,
           own, far, z_send, z_recv, c_send, c_recv,
           w_sem, t_sem, route_ssem, route_rsem, i_ssem, i_rsem, r_ssem, r_rsem, h_ssem, h_rsem, z_ssem, z_rsem, c_ssem, c_rsem):
    src, local, cap, width = x_hbm.shape
    top, tokens = slot_hbm.shape
    ff = wg_hbm.shape[2]
    rows = src * cap
    span = local * cap
    block = inner * span
    piece = width // CHUNKS
    split = INNER_CHUNKS * piece
    mixed = MIXED[0] * piece
    o = lax.axis_index("outer")
    i = lax.axis_index("expert")
    middle = lax.rem((o + 1) // 2, 2)
    half = o // 2
    seat = lax.rem(o, 2)
    near = o + 1 - 2 * seat
    across = (2 - half, 3 - 3 * half)

    def inner_peer(r):
        return lax.rem(i + r, inner)

    def outer_peer(r):
        return lax.rem(o + r, outer)

    def weight_copy(e, kind):
        s = lax.rem(e, SLOTS)
        hbm, buf = ((wg_hbm, wg_buf), (wu_hbm, wu_buf), (wd_hbm, wd_buf))[kind]
        return pltpu.make_async_copy(hbm.at[e], buf.at[s], w_sem.at[kind, s])

    def x_copy(e):
        s = lax.rem(e, SLOTS)
        return pltpu.make_async_copy(x_hbm.at[:, e], x_buf.at[s], w_sem.at[3, s])

    def fetch(e, kind):
        @pl.when(e < local)
        def _():
            if kind == 0:
                x_copy(e).start()
            weight_copy(e, kind).start()

    def arrived(e, kind):
        if kind == 0:
            x_copy(e).wait()
        weight_copy(e, kind).wait()
        fetch(e + (kind + WINDOW) // 3, (kind + WINDOW) % 3)

    def inner_copy(src_ref, dst_ref, n, r):
        return pltpu.make_async_remote_copy(
            src_ref=src_ref, dst_ref=dst_ref, send_sem=i_ssem.at[n, r - 1], recv_sem=i_rsem.at[n, r - 1],
            device_id={"expert": inner_peer(r)}, device_id_type=MESH)

    def chunk_cols(n):
        return pl.ds(n * piece, piece)

    def blocks(n):
        return pl.ds(2 * (1 - half), 2) if n in MIXED else pl.ds(0, outer)

    def send_inner(e, n):
        for r in range(1, inner):
            inner_copy(in_send.at[n, e, inner_peer(r), blocks(n)], y_in.at[n, i, e, blocks(n)], n, r).start()

    def all_inner(n, r):
        return inner_copy(in_send.at[n, :, inner_peer(r), blocks(n)],
                          y_in.at[n, lax.rem(i + inner - r, inner), :, blocks(n)], n, r)

    def outer_copy(src_ref, dst_ref, r):
        return pltpu.make_async_remote_copy(
            src_ref=src_ref, dst_ref=dst_ref, send_sem=r_ssem.at[r - 1], recv_sem=r_rsem.at[r - 1],
            device_id={"outer": outer_peer(r)}, device_id_type=MESH)

    def send_outer(e):
        for r in range(1, outer):
            outer_copy(out_send.at[e, outer_peer(r)], y_out.at[o, e], r).start()

    def all_outer(r):
        return outer_copy(out_send.at[:, outer_peer(r)], y_out.at[lax.rem(o + outer - r, outer)], r)

    def half_copy(src_ref, dst_ref):
        return pltpu.make_async_remote_copy(
            src_ref=src_ref, dst_ref=dst_ref, send_sem=h_ssem, recv_sem=h_rsem,
            device_id={"outer": near}, device_id_type=MESH)

    def send_half(e):
        half_copy(half_send.at[e, near - 2 * half], y_half.at[seat, e]).start()

    def all_half():
        return half_copy(half_send.at[:, near - 2 * half], y_half.at[1 - seat])

    def copy_z(p, q, slot, peer):
        return pltpu.make_async_remote_copy(
            src_ref=z_send.at[q, p], dst_ref=z_recv.at[slot, p],
            send_sem=z_ssem.at[q, p], recv_sem=z_rsem.at[slot, p],
            device_id={"outer": peer}, device_id_type=MESH)

    def copy_near(p):
        return copy_z(p, 0, 0, near)

    def copy_across(p, k):
        return copy_z(p, 1 + k, middle + (1 - middle) * (2 + k), middle * across[k] + (1 - middle) * near)

    def copy_c(p, r):
        return pltpu.make_async_remote_copy(
            src_ref=c_send.at[r - 1, p], dst_ref=c_recv.at[r - 1, p],
            send_sem=c_ssem.at[r - 1, p], recv_sem=c_rsem.at[r - 1, p],
            device_id={"expert": inner_peer(r)}, device_id_type=MESH)

    def copy_route(q):
        if q < outer - 1:
            dst, peer = route.at[o], {"outer": outer_peer(q + 1)}
        else:
            dst, peer = route.at[outer + i], {"expert": inner_peer(q - outer + 2)}
        return pltpu.make_async_remote_copy(
            src_ref=route_send, dst_ref=dst, send_sem=route_ssem.at[q], recv_sem=route_rsem.at[q],
            device_id=peer, device_id_type=MESH)

    small = [pltpu.make_async_copy(a, b, t_sem.at[k]) for k, (a, b) in enumerate(
        ((slot_hbm, slot_ref), (ids_hbm, ids_ref), (gate_hbm, gate_ref)))]
    for c in small:
        c.start()
    for k in range(WINDOW):
        fetch(k // 3, k % 3)
    peers = outer + inner - 2
    barrier = pltpu.get_barrier_semaphore()
    for r in range(1, outer):
        pl.semaphore_signal(barrier, inc=1, device_id={"outer": outer_peer(r)}, device_id_type=MESH)
    for r in range(1, inner):
        pl.semaphore_signal(barrier, inc=1, device_id={"expert": inner_peer(r)}, device_id_type=MESH)

    for c in small:
        c.wait()
    slot = slot_ref[...]
    flat = jnp.where(slot >= 0, ids_ref[...] * cap + slot, -1).astype(F32)
    lanes = jnp.concatenate([flat, gate_ref[...]], axis=0)
    route_send[...] = lanes
    route[o] = lanes
    route[outer + i] = lanes
    pl.semaphore_wait(barrier, peers)
    for q in range(peers):
        copy_route(q).start()

    row = lax.broadcasted_iota(jnp.int32, (block, tokens), 0)
    row_in = o * block + row
    row_out = (row // span) * block + i * span + row % span

    def build_pick(k):
        want = jnp.where(k < outer, row_in, row_out).astype(F32)
        gates = jnp.zeros((block, tokens), F32)
        hits = jnp.zeros((block, tokens), F32)
        for j in range(top):
            hit = want == route[k, j:j + 1, :]
            gates = jnp.where(hit, route[k, top + j:top + j + 1, :], gates)
            hits = jnp.where(hit, 1.0, hits)
        used[k] = jnp.broadcast_to(jnp.max(hits, axis=1, keepdims=True), (block, tokens)).astype(BF16)
        g = gates.T
        high = jnp.minimum(g, BF16_MAX).astype(BF16)
        rest = g - high.astype(F32)
        mid = rest.astype(BF16)
        low = (rest - mid.astype(F32)).astype(BF16)
        pick[k, 0:tokens] = high
        pick[k, tokens:2 * tokens] = mid
        pick[k, 2 * tokens:3 * tokens] = low

    def expert_step(e, carry):
        s = lax.rem(e, SLOTS)
        arrived(e, 0)
        arrived(e, 1)
        x = x_buf[s].reshape(rows, width)
        tile = 256
        for n in range(ff // tile):
            cols = pl.ds(n * tile, tile)
            gate = jnp.dot(x, wg_buf[s, :, cols], preferred_element_type=F32)
            up = jnp.dot(x, wu_buf[s, :, cols], preferred_element_type=F32)
            h_buf[:, cols] = (gate * lax.logistic(gate) * up).astype(BF16)
        arrived(e, 2)
        h = h_buf[...]

        def down(n):
            y = jnp.dot(h, wd_buf[s, :, chunk_cols(n)], preferred_element_type=F32).astype(BF16)
            return y.reshape(outer, inner, cap, piece)

        for n in OUTER:
            out_send[e, :, :, :, pl.ds((n - OUTER[0]) * piece, piece)] = down(n)
        for n in MIXED:
            y = down(n)
            for k in range(inner):
                in_send[n, e, k] = y[:, k]
            cols = pl.ds((n - MIXED[0]) * piece, piece)

            @pl.when(half == 0)
            def _():
                half_send[e, :, :, :, cols] = y[0:2]

            @pl.when(half == 1)
            def _():
                half_send[e, :, :, :, cols] = y[2:4]
        send_outer(e)
        for n in FIRST + (LATER,):
            y = down(n)
            for k in range(inner):
                in_send[n, e, k] = y[:, k]
            if n == FIRST[0]:
                send_half(e)
            else:
                send_inner(e, n - 1)
        y_in[:, i, e] = in_send[:, e, i]
        y_out[o, e] = out_send[e, o]
        y_half[seat, e] = half_send[e, seat]

        @pl.when(e == 0)
        def _():
            for q in range(peers):
                copy_route(q).wait_recv()

        build_pick(e)
        return carry

    lax.fori_loop(0, local, expert_step, 0)

    for n in (LATER,) + MIXED:
        def send_last(e, carry):
            send_inner(e, n)
            return carry

        lax.fori_loop(0, local, send_last, 0)

    def partial_sum(k, slots, y):
        mask = jnp.concatenate([used[k, slots]] * (piece // tokens), axis=1) > 0
        y = jnp.where(mask, y, jnp.zeros((), BF16))
        s = jnp.dot(pick[k, :, slots], y, preferred_element_type=F32)
        return s[0:tokens] + s[tokens:2 * tokens] + s[2 * tokens:3 * tokens]

    def block_sum(n, k):
        return partial_sum(k, pl.ds(0, block), y_in[n, :, :, k].reshape(block, piece))

    def half_sum(n, k):
        y = y_half[:, :, k, :, pl.ds(n * piece - mixed, piece)].reshape(2 * span, piece)
        return partial_sum(outer + k, pl.ds(pl.multiple_of(half * 2 * span, 2 * span), 2 * span), y)

    def outer_sum(n, k):
        y = y_out[:, :, k, :, pl.ds(n * piece - split, piece)].reshape(block, piece)
        return partial_sum(outer + k, pl.ds(0, block), y)

    def sum_across(n):
        for r in range(1, inner):
            all_inner(n, r).wait_recv()
        for k in (1, 0):
            total = block_sum(n, across[k])

            @pl.when(middle == 1)
            def _():
                far[k, :, chunk_cols(n)] = total

            @pl.when(middle == 0)
            def _():
                z_send[1 + k, n] = total.astype(BF16)
                copy_across(n, k).start()

    def sum_near(n):
        z_send[0, n] = block_sum(n, near).astype(BF16)
        copy_near(n).start()

    def sum_inner(n, of):
        for r in range(1, inner):
            c_send[r - 1, n - MIXED[0]] = of(n, inner_peer(r)).astype(BF16)
            copy_c(n - MIXED[0], r).start()
        own[:, chunk_cols(n)] = of(n, i)

    def pass_on(n):
        @pl.when(middle == 1)
        def _():
            for k in (1, 0):
                copy_z(n, 1 + k, 2 + k, near).wait_recv()
                z_send[1 + k, n] = (far[k, :, chunk_cols(n)] + z_recv[2 + k, n].astype(F32)).astype(BF16)
                copy_across(n, k).start()

    def finish(n):
        total = own[:, chunk_cols(n)]
        if n < MIXED[0]:
            copy_z(n, 0, 0, near).wait_recv()
            total = total + z_recv[0, n].astype(F32)
        else:
            for r in range(1, inner):
                copy_c(n - MIXED[0], r).wait_recv()
                total = total + c_recv[r - 1, n - MIXED[0]].astype(F32)
        if n < INNER_CHUNKS:
            copy_z(n, 1, 1, near).wait_recv()
            total = total + z_recv[1, n].astype(F32)
        out_ref[:, chunk_cols(n)] = total.astype(BF16)

    for n in FIRST:
        sum_across(n)
    for r in range(1, outer):
        all_outer(r).wait_recv()
    all_half().wait_recv()
    for n in OUTER:
        sum_inner(n, outer_sum)
    for n in MIXED:
        sum_inner(n, half_sum)
    pass_on(0)
    sum_across(3)
    pass_on(1)
    sum_across(4)
    pass_on(2)
    sum_across(5)
    for n in FIRST + (LATER,):
        sum_near(n)
    pass_on(3)
    for n in FIRST + (LATER,):
        own[:, chunk_cols(n)] = block_sum(n, o)
    pass_on(4)
    pass_on(5)

    for q in range(peers):
        copy_route(q).wait_send()
    for r in range(1, inner):
        for n in range(INNER_CHUNKS):
            all_inner(n, r).wait_send()
    for r in range(1, outer):
        all_outer(r).wait_send()
    all_half().wait_send()
    for n in OUTER + MIXED:
        finish(n)
    for n in FIRST + (LATER,):
        finish(n)
    for n in OUTER + MIXED:
        for r in range(1, inner):
            copy_c(n - MIXED[0], r).wait_send()
    for n in range(INNER_CHUNKS):
        if n < MIXED[0]:
            copy_near(n).wait_send()
        for k in (1, 0):
            copy_across(n, k).wait_send()


def solution(mesh):
    outer = mesh.shape["outer"]
    inner = mesh.shape["expert"]

    def local_step(x_disp, w_gate, w_up, w_down, slot_idx, expert_ids, gate_wts):
        src, local, cap, width = x_disp.shape
        tokens, top = slot_idx.shape
        ff = w_gate.shape[2]
        block = inner * local * cap
        sources = outer + inner
        piece = width // CHUNKS
        split = INNER_CHUNKS * piece
        turned = CHUNKS - MIXED[0]
        peers = outer + inner - 2
        dma = pltpu.SemaphoreType.DMA
        hbm = pl.BlockSpec(memory_space=pltpu.HBM)
        vmem = pl.BlockSpec(memory_space=pltpu.VMEM)
        return pl.pallas_call(
            functools.partial(kernel, outer, inner),
            out_shape=jax.ShapeDtypeStruct((tokens, width), BF16),
            in_specs=[hbm] * 7,
            out_specs=vmem,
            scratch_shapes=[
                pltpu.VMEM((SLOTS, src, cap, width), BF16),
                pltpu.VMEM((SLOTS, width, ff), BF16),
                pltpu.VMEM((SLOTS, width, ff), BF16),
                pltpu.VMEM((SLOTS, ff, width), BF16),
                pltpu.VMEM((src * cap, ff), BF16),
                pltpu.VMEM((INNER_CHUNKS, local, inner, outer, cap, piece), BF16),
                pltpu.VMEM((local, outer, inner, cap, width - split), BF16),
                pltpu.VMEM((local, 2, inner, cap, len(MIXED) * piece), BF16),
                pltpu.VMEM((INNER_CHUNKS, inner, local, outer, cap, piece), BF16),
                pltpu.VMEM((outer, local, inner, cap, width - split), BF16),
                pltpu.VMEM((2, local, inner, cap, len(MIXED) * piece), BF16),
                pltpu.VMEM((top, tokens), jnp.int32),
                pltpu.VMEM((top, tokens), jnp.int32),
                pltpu.VMEM((top, tokens), F32),
                pltpu.VMEM((2 * top, tokens), F32),
                pltpu.VMEM((sources, 2 * top, tokens), F32),
                pltpu.VMEM((sources, 3 * tokens, block), BF16),
                pltpu.VMEM((sources, block, tokens), BF16),
                pltpu.VMEM((tokens, width), F32),
                pltpu.VMEM((2, tokens, split), F32),
                pltpu.VMEM((3, INNER_CHUNKS, tokens, piece), BF16),
                pltpu.VMEM((4, INNER_CHUNKS, tokens, piece), BF16),
                pltpu.VMEM((inner - 1, turned, tokens, piece), BF16),
                pltpu.VMEM((inner - 1, turned, tokens, piece), BF16),
                dma((4, SLOTS)), dma((3,)),
                dma((peers,)), dma((peers,)),
                dma((INNER_CHUNKS, inner - 1)), dma((INNER_CHUNKS, inner - 1)),
                dma((outer - 1,)), dma((outer - 1,)),
                dma, dma,
                dma((3, INNER_CHUNKS)), dma((4, INNER_CHUNKS)),
                dma((inner - 1, turned)), dma((inner - 1, turned)),
            ],
            compiler_params=pltpu.CompilerParams(
                collective_id=0, has_side_effects=True, vmem_limit_bytes=54_000_000),
        )(x_disp, w_gate, w_up, w_down, *(pltpu.with_memory_space_constraint(a.T, pltpu.HBM) for a in (slot_idx, expert_ids, gate_wts)))

    expert_spec = P(("outer", "expert"))
    token_spec = P(("data", "outer", "expert"))
    return jax.shard_map(local_step, mesh=mesh, in_specs=(P("data", ("outer", "expert")), expert_spec, expert_spec, expert_spec, token_spec, token_spec, token_spec), out_specs=token_spec, check_vma=False)
```

```python
import functools

import jax
import jax.numpy as jnp
from jax import lax
from jax.experimental import pallas as pl
from jax.experimental.pallas import tpu as pltpu
from jax.sharding import PartitionSpec as P

MESH = pl.DeviceIdType.MESH
F32 = jnp.float32
BF16 = jnp.bfloat16
SLOTS = 3
WINDOW = 4
BF16_MAX = 3.3895313892515355e38


CHUNKS = 8
FIRST = (0, 1, 2)
LATER = 3
MIXED = (4, 5)
OUTER = (6, 7)
INNER_CHUNKS = 6


def kernel(outer, inner, x_hbm, wg_hbm, wu_hbm, wd_hbm, slot_hbm, ids_hbm, gate_hbm, out_ref,
           x_buf, wg_buf, wu_buf, wd_buf, h_buf, y_send, y_in, y_out, y_half, slot_ref, ids_ref, gate_ref, route_send, route, pick, used,
           own, far, z_send, z_recv, c_send, c_recv,
           w_sem, t_sem, route_ssem, route_rsem, i_ssem, i_rsem, r_ssem, r_rsem, h_ssem, h_rsem, z_ssem, z_rsem, c_ssem, c_rsem):
    src, local, cap, width = x_hbm.shape
    top, tokens = slot_hbm.shape
    ff = wg_hbm.shape[2]
    rows = src * cap
    span = local * cap
    block = inner * span
    piece = width // CHUNKS
    split = INNER_CHUNKS * piece
    mixed = MIXED[0] * piece
    o = lax.axis_index("outer")
    i = lax.axis_index("expert")
    middle = lax.rem((o + 1) // 2, 2)
    half = o // 2
    seat = lax.rem(o, 2)
    near = o + 1 - 2 * seat
    across = (2 - half, 3 - 3 * half)

    def inner_peer(r):
        return lax.rem(i + r, inner)

    def outer_peer(r):
        return lax.rem(o + r, outer)

    def weight_copy(e, kind):
        s = lax.rem(e, SLOTS)
        hbm, buf = ((wg_hbm, wg_buf), (wu_hbm, wu_buf), (wd_hbm, wd_buf))[kind]
        return pltpu.make_async_copy(hbm.at[e], buf.at[s], w_sem.at[kind, s])

    def x_copy(e):
        s = lax.rem(e, SLOTS)
        return pltpu.make_async_copy(x_hbm.at[:, e], x_buf.at[s], w_sem.at[3, s])

    def fetch(e, kind):
        @pl.when(e < local)
        def _():
            if kind == 0:
                x_copy(e).start()
            weight_copy(e, kind).start()

    def arrived(e, kind):
        if kind == 0:
            x_copy(e).wait()
        weight_copy(e, kind).wait()
        fetch(e + (kind + WINDOW) // 3, (kind + WINDOW) % 3)

    def inner_copy(src_ref, dst_ref, n, r):
        return pltpu.make_async_remote_copy(
            src_ref=src_ref, dst_ref=dst_ref, send_sem=i_ssem.at[n, r - 1], recv_sem=i_rsem.at[n, r - 1],
            device_id={"expert": inner_peer(r)}, device_id_type=MESH)

    def chunk_cols(n):
        return pl.ds(n * piece, piece)

    def blocks(n):
        return pl.ds(2 * (1 - half), 2) if n in MIXED else pl.ds(0, outer)

    def send_inner(e, n):
        for r in range(1, inner):
            inner_copy(y_send.at[e, blocks(n), inner_peer(r), :, chunk_cols(n)],
                       y_in.at[blocks(n), i, e, :, chunk_cols(n)], n, r).start()

    def all_inner(n, r):
        return inner_copy(y_send.at[:, blocks(n), inner_peer(r), :, chunk_cols(n)],
                          y_in.at[blocks(n), lax.rem(i + inner - r, inner), :, :, chunk_cols(n)], n, r)

    def outer_copy(src_ref, dst_ref, r):
        return pltpu.make_async_remote_copy(
            src_ref=src_ref, dst_ref=dst_ref, send_sem=r_ssem.at[r - 1], recv_sem=r_rsem.at[r - 1],
            device_id={"outer": outer_peer(r)}, device_id_type=MESH)

    rest_cols = pl.ds(split, width - split)

    def send_outer(e):
        for r in range(1, outer):
            outer_copy(y_send.at[e, outer_peer(r), :, :, rest_cols], y_out.at[:, o, e], r).start()

    def all_outer(r):
        return outer_copy(y_send.at[:, outer_peer(r), :, :, rest_cols], y_out.at[:, lax.rem(o + outer - r, outer)], r)

    half_cols = pl.ds(mixed, split - mixed)

    def half_copy(src_ref, dst_ref):
        return pltpu.make_async_remote_copy(
            src_ref=src_ref, dst_ref=dst_ref, send_sem=h_ssem, recv_sem=h_rsem,
            device_id={"outer": near}, device_id_type=MESH)

    def send_half(e):
        half_copy(y_send.at[e, near, :, :, half_cols], y_half.at[:, seat, e]).start()

    def all_half():
        return half_copy(y_send.at[:, near, :, :, half_cols], y_half.at[:, 1 - seat])

    def copy_z(p, q, slot, peer):
        return pltpu.make_async_remote_copy(
            src_ref=z_send.at[q, p], dst_ref=z_recv.at[slot, p],
            send_sem=z_ssem.at[q, p], recv_sem=z_rsem.at[slot, p],
            device_id={"outer": peer}, device_id_type=MESH)

    def copy_near(p):
        return copy_z(p, 0, 0, near)

    def copy_across(p, k):
        return copy_z(p, 1 + k, middle + (1 - middle) * (2 + k), middle * across[k] + (1 - middle) * near)

    def copy_c(p, r):
        return pltpu.make_async_remote_copy(
            src_ref=c_send.at[r - 1, p], dst_ref=c_recv.at[r - 1, p],
            send_sem=c_ssem.at[r - 1, p], recv_sem=c_rsem.at[r - 1, p],
            device_id={"expert": inner_peer(r)}, device_id_type=MESH)

    def copy_route(q):
        if q < outer - 1:
            dst, peer = route.at[o], {"outer": outer_peer(q + 1)}
        else:
            dst, peer = route.at[outer + i], {"expert": inner_peer(q - outer + 2)}
        return pltpu.make_async_remote_copy(
            src_ref=route_send, dst_ref=dst, send_sem=route_ssem.at[q], recv_sem=route_rsem.at[q],
            device_id=peer, device_id_type=MESH)

    small = [pltpu.make_async_copy(a, b, t_sem.at[k]) for k, (a, b) in enumerate(
        ((slot_hbm, slot_ref), (ids_hbm, ids_ref), (gate_hbm, gate_ref)))]
    for c in small:
        c.start()
    for k in range(WINDOW):
        fetch(k // 3, k % 3)
    peers = outer + inner - 2
    barrier = pltpu.get_barrier_semaphore()
    for r in range(1, outer):
        pl.semaphore_signal(barrier, inc=1, device_id={"outer": outer_peer(r)}, device_id_type=MESH)
    for r in range(1, inner):
        pl.semaphore_signal(barrier, inc=1, device_id={"expert": inner_peer(r)}, device_id_type=MESH)

    for c in small:
        c.wait()
    slot = slot_ref[...]
    flat = jnp.where(slot >= 0, ids_ref[...] * cap + slot, -1).astype(F32)
    lanes = jnp.concatenate([flat, gate_ref[...]], axis=0)
    route_send[...] = lanes
    route[o] = lanes
    route[outer + i] = lanes
    pl.semaphore_wait(barrier, peers)
    for q in range(peers):
        copy_route(q).start()

    row = lax.broadcasted_iota(jnp.int32, (block, tokens), 0)
    row_in = o * block + row
    row_out = (row // span) * block + i * span + row % span

    def build_pick(k):
        want = jnp.where(k < outer, row_in, row_out).astype(F32)
        gates = jnp.zeros((block, tokens), F32)
        hits = jnp.zeros((block, tokens), F32)
        for j in range(top):
            hit = want == route[k, j:j + 1, :]
            gates = jnp.where(hit, route[k, top + j:top + j + 1, :], gates)
            hits = jnp.where(hit, 1.0, hits)
        used[k] = jnp.broadcast_to(jnp.max(hits, axis=1, keepdims=True), (block, tokens)).astype(BF16)
        g = gates.T
        high = jnp.minimum(g, BF16_MAX).astype(BF16)
        rest = g - high.astype(F32)
        mid = rest.astype(BF16)
        low = (rest - mid.astype(F32)).astype(BF16)
        pick[k, 0:tokens] = high
        pick[k, tokens:2 * tokens] = mid
        pick[k, 2 * tokens:3 * tokens] = low

    def expert_step(e, carry):
        s = lax.rem(e, SLOTS)
        arrived(e, 0)
        arrived(e, 1)
        x = x_buf[s].reshape(rows, width)
        tile = 256
        for n in range(ff // tile):
            cols = pl.ds(n * tile, tile)
            gate = jnp.dot(x, wg_buf[s, :, cols], preferred_element_type=F32)
            up = jnp.dot(x, wu_buf[s, :, cols], preferred_element_type=F32)
            h_buf[:, cols] = (gate * lax.logistic(gate) * up).astype(BF16)
        arrived(e, 2)
        h = h_buf[...]

        def down(*numbers):
            for n in numbers:
                y = jnp.dot(h, wd_buf[s, :, chunk_cols(n)], preferred_element_type=F32).astype(BF16)
                y_send[e, :, :, :, chunk_cols(n)] = y.reshape(outer, inner, cap, piece)

        down(0, 1)
        send_inner(e, 0)
        down(2)
        send_inner(e, 1)
        down(6, 7)
        send_inner(e, 2)
        down(4)
        send_outer(e)
        down(5, 3)
        send_half(e)
        y_in[:, i, e] = y_send[e, :, i, :, 0:split]
        y_out[:, o, e] = y_send[e, o, :, :, split:]
        y_half[:, seat, e] = y_send[e, o, :, :, mixed:split]

        @pl.when(e == 0)
        def _():
            for q in range(peers):
                copy_route(q).wait_recv()

        build_pick(e)
        return carry

    lax.fori_loop(0, local, expert_step, 0)

    for n in (LATER,) + MIXED:
        def send_last(e, carry):
            send_inner(e, n)
            return carry

        lax.fori_loop(0, local, send_last, 0)

    def partial_sum(k, slots, y):
        mask = jnp.concatenate([used[k, slots]] * (piece // tokens), axis=1) > 0
        y = jnp.where(mask, y, jnp.zeros((), BF16))
        s = jnp.dot(pick[k, :, slots], y, preferred_element_type=F32)
        return s[0:tokens] + s[tokens:2 * tokens] + s[2 * tokens:3 * tokens]

    def block_sum(n, k):
        return partial_sum(k, pl.ds(0, block), y_in[k, :, :, :, chunk_cols(n)].reshape(block, piece))

    def half_sum(n, k):
        y = y_half[k, :, :, :, pl.ds(n * piece - mixed, piece)].reshape(2 * span, piece)
        return partial_sum(outer + k, pl.ds(pl.multiple_of(half * 2 * span, 2 * span), 2 * span), y)

    def outer_sum(n, k):
        y = y_out[k, :, :, :, pl.ds(n * piece - split, piece)].reshape(block, piece)
        return partial_sum(outer + k, pl.ds(0, block), y)

    def sum_across(n):
        for r in range(1, inner):
            all_inner(n, r).wait_recv()
        for k in (1, 0):
            total = block_sum(n, across[k])

            @pl.when(middle == 1)
            def _():
                far[k, :, chunk_cols(n)] = total

            @pl.when(middle == 0)
            def _():
                z_send[1 + k, n] = total.astype(BF16)
                copy_across(n, k).start()

    def sum_near(n):
        z_send[0, n] = block_sum(n, near).astype(BF16)
        copy_near(n).start()

    def sum_inner(n, of):
        for r in range(1, inner):
            c_send[r - 1, n - MIXED[0]] = of(n, inner_peer(r)).astype(BF16)
            copy_c(n - MIXED[0], r).start()
        own[:, chunk_cols(n)] = of(n, i)

    def pass_on(n):
        @pl.when(middle == 1)
        def _():
            for k in (1, 0):
                copy_z(n, 1 + k, 2 + k, near).wait_recv()
                z_send[1 + k, n] = (far[k, :, chunk_cols(n)] + z_recv[2 + k, n].astype(F32)).astype(BF16)
                copy_across(n, k).start()

    def finish(n):
        total = own[:, chunk_cols(n)]
        if n < MIXED[0]:
            copy_z(n, 0, 0, near).wait_recv()
            total = total + z_recv[0, n].astype(F32)
        else:
            for r in range(1, inner):
                copy_c(n - MIXED[0], r).wait_recv()
                total = total + c_recv[r - 1, n - MIXED[0]].astype(F32)
        if n < INNER_CHUNKS:
            copy_z(n, 1, 1, near).wait_recv()
            total = total + z_recv[1, n].astype(F32)
        out_ref[:, chunk_cols(n)] = total.astype(BF16)

    for n in FIRST:
        sum_across(n)
    for r in range(1, outer):
        all_outer(r).wait_recv()
    all_half().wait_recv()
    for n in OUTER:
        sum_inner(n, outer_sum)
    for n in MIXED:
        sum_inner(n, half_sum)
    pass_on(0)
    sum_across(3)
    pass_on(1)
    sum_across(4)
    pass_on(2)
    sum_across(5)
    for n in FIRST + (LATER,):
        sum_near(n)
    pass_on(3)
    for n in FIRST + (LATER,):
        own[:, chunk_cols(n)] = block_sum(n, o)
    pass_on(4)
    pass_on(5)

    for q in range(peers):
        copy_route(q).wait_send()
    for r in range(1, inner):
        for n in range(INNER_CHUNKS):
            all_inner(n, r).wait_send()
    for r in range(1, outer):
        all_outer(r).wait_send()
    all_half().wait_send()
    for n in OUTER + MIXED:
        finish(n)
    for n in FIRST + (LATER,):
        finish(n)
    for n in OUTER + MIXED:
        for r in range(1, inner):
            copy_c(n - MIXED[0], r).wait_send()
    for n in range(INNER_CHUNKS):
        if n < MIXED[0]:
            copy_near(n).wait_send()
        for k in (1, 0):
            copy_across(n, k).wait_send()


def solution(mesh):
    outer = mesh.shape["outer"]
    inner = mesh.shape["expert"]

    def local_step(x_disp, w_gate, w_up, w_down, slot_idx, expert_ids, gate_wts):
        src, local, cap, width = x_disp.shape
        tokens, top = slot_idx.shape
        ff = w_gate.shape[2]
        block = inner * local * cap
        sources = outer + inner
        piece = width // CHUNKS
        split = INNER_CHUNKS * piece
        turned = CHUNKS - MIXED[0]
        peers = outer + inner - 2
        dma = pltpu.SemaphoreType.DMA
        hbm = pl.BlockSpec(memory_space=pltpu.HBM)
        vmem = pl.BlockSpec(memory_space=pltpu.VMEM)
        return pl.pallas_call(
            functools.partial(kernel, outer, inner),
            out_shape=jax.ShapeDtypeStruct((tokens, width), BF16),
            in_specs=[hbm] * 7,
            out_specs=vmem,
            scratch_shapes=[
                pltpu.VMEM((SLOTS, src, cap, width), BF16),
                pltpu.VMEM((SLOTS, width, ff), BF16),
                pltpu.VMEM((SLOTS, width, ff), BF16),
                pltpu.VMEM((SLOTS, ff, width), BF16),
                pltpu.VMEM((src * cap, ff), BF16),
                pltpu.VMEM((local, outer, inner, cap, width), BF16),
                pltpu.VMEM((outer, inner, local, cap, split), BF16),
                pltpu.VMEM((inner, outer, local, cap, width - split), BF16),
                pltpu.VMEM((inner, 2, local, cap, len(MIXED) * piece), BF16),
                pltpu.VMEM((top, tokens), jnp.int32),
                pltpu.VMEM((top, tokens), jnp.int32),
                pltpu.VMEM((top, tokens), F32),
                pltpu.VMEM((2 * top, tokens), F32),
                pltpu.VMEM((sources, 2 * top, tokens), F32),
                pltpu.VMEM((sources, 3 * tokens, block), BF16),
                pltpu.VMEM((sources, block, tokens), BF16),
                pltpu.VMEM((tokens, width), F32),
                pltpu.VMEM((2, tokens, split), F32),
                pltpu.VMEM((3, INNER_CHUNKS, tokens, piece), BF16),
                pltpu.VMEM((4, INNER_CHUNKS, tokens, piece), BF16),
                pltpu.VMEM((inner - 1, turned, tokens, piece), BF16),
                pltpu.VMEM((inner - 1, turned, tokens, piece), BF16),
                dma((4, SLOTS)), dma((3,)),
                dma((peers,)), dma((peers,)),
                dma((INNER_CHUNKS, inner - 1)), dma((INNER_CHUNKS, inner - 1)),
                dma((outer - 1,)), dma((outer - 1,)),
                dma, dma,
                dma((3, INNER_CHUNKS)), dma((4, INNER_CHUNKS)),
                dma((inner - 1, turned)), dma((inner - 1, turned)),
            ],
            compiler_params=pltpu.CompilerParams(
                collective_id=0, has_side_effects=True, vmem_limit_bytes=54_000_000),
        )(x_disp, w_gate, w_up, w_down, *(pltpu.with_memory_space_constraint(a.T, pltpu.HBM) for a in (slot_idx, expert_ids, gate_wts)))

    expert_spec = P(("outer", "expert"))
    token_spec = P(("data", "outer", "expert"))
    return jax.shard_map(local_step, mesh=mesh, in_specs=(P("data", ("outer", "expert")), expert_spec, expert_spec, expert_spec, token_spec, token_spec, token_spec), out_specs=token_spec, check_vma=False)
```
